32 devices in a mesh: freq: 4 (over z), trace: 8 (over y, x, core).
Axes of the slice: x: 2, y: 2, z: 4, core: 2. Of those that a mesh axis runs over, the one named last changes fastest.
Arguments:
- recorded: float32 [8, 2, 2048, 1024], P(None, None, 'freq', 'trace'), may hold values from -16 to 16
- multiples: float32 [8, 2, 2048, 1024], P(None, None, 'freq', 'trace'), may hold values from -6 to 6
Outputs:
- primaries: float32 [8, 2, 2048, 1024], P(None, None, 'freq', 'trace')
- filters: float32 [8, 2, 32, 64], P(None, None, 'freq')
The draws below stay inside these ranges and needn't reach their ends.
All inputs are finite; a program needn't handle non-finite values.
Results may differ from the reference program's by a relative error of at most 0.0001.
Values sent between devices are 32-bit elements; how exact they have to be, the bound alone decides.
A program may use at most 128 MiB of HBM per device.

```python
import jax
import jax.numpy as jnp
from jax import lax

SHOTS = 8
NF = 2048
FB = 64
TAPS = 64
ITERS = 3
NX = 1024
NB = 32
N_TRACE = 8


def paired_fields(key):
    key_mult, key_smooth, key_noise, key_first, key_second = jax.random.split(jax.random.fold_in(key, 17), 5)
    white_part = jax.random.normal(key_mult, (SHOTS, 2, NF, NX), jnp.float32)
    base_field = jax.random.normal(key_smooth, (SHOTS, 2, NF, NX), jnp.float32)
    smooth_part = base_field
    for offset in range(1, 12):
        smooth_part = smooth_part + jnp.roll(base_field, offset, axis=3)
    smooth_part = smooth_part * 0.28867513
    mult_field = jnp.clip((white_part + 2.0 * smooth_part) * 0.4472136, -6.0, 6.0)
    noise_part = jnp.clip(jax.random.normal(key_noise, (SHOTS, 2, NF, NX), jnp.float32), -4.0, 4.0)
    first_gain = jax.random.uniform(key_first, (SHOTS, 2, NF, 1), jnp.float32, -1.0, 1.0)
    second_gain = jax.random.uniform(key_second, (SHOTS, 2, NF, 1), jnp.float32, -0.6, 0.6)
    shifted = jnp.roll(mult_field, 1, axis=3)
    real_part = first_gain[:, 0] * mult_field[:, 0] - first_gain[:, 1] * mult_field[:, 1] + second_gain[:, 0] * shifted[:, 0] - second_gain[:, 1] * shifted[:, 1]
    imag_part = first_gain[:, 0] * mult_field[:, 1] + first_gain[:, 1] * mult_field[:, 0] + second_gain[:, 0] * shifted[:, 1] + second_gain[:, 1] * shifted[:, 0]
    recorded_field = jnp.clip(noise_part + jnp.stack([real_part, imag_part], axis=1), -16.0, 16.0)
    return (recorded_field, mult_field)


def draw_recorded(key, part):
    return paired_fields(key)[0]


def draw_multiples(key, part):
    return paired_fields(key)[1]


def setup_inputs(seed: int = 0) -> dict:
    key_of = jax.random.split(jax.random.key(seed), 3)
    recorded = draw_recorded(jax.random.fold_in(key_of[2], 71), 0)
    multiples = draw_multiples(jax.random.fold_in(key_of[2], 71), 0)
    return dict(recorded=recorded, multiples=multiples)


def toeplitz_rows(taps_vec, trace_rows):
    tap_count = taps_vec.shape[-1]
    window_len = trace_rows + tap_count
    leading = taps_vec.shape[:-1]
    padded = jnp.concatenate([jnp.zeros(leading + (1,), jnp.float32), taps_vec[..., ::-1], jnp.zeros(leading + (trace_rows,), jnp.float32)], -1)
    repeated = jnp.tile(padded, (1,) * len(leading) + (trace_rows,))
    return repeated[..., :trace_rows * window_len].reshape(leading + (trace_rows, window_len))


def product(left, right):
    return jnp.einsum('bfj,bxj->bfx', left, right, precision=lax.Precision.HIGHEST)


def correlate(left, right):
    return jnp.einsum('bfj,bfx->bxj', left, right, precision=lax.Precision.HIGHEST)


def forward_one(window, taps_vec):
    trace_rows = window.shape[-1] - taps_vec.shape[-1]
    toeplitz = toeplitz_rows(taps_vec, trace_rows)
    real_part = product(window[0], toeplitz[0]) - product(window[1], toeplitz[1])
    imag_part = product(window[0], toeplitz[1]) + product(window[1], toeplitz[0])
    return jnp.stack([real_part, imag_part])


def adjoint_one(window, residual, tap_count):
    real_part = correlate(window[0], residual[0]) + correlate(window[1], residual[1])
    imag_part = correlate(window[0], residual[1]) - correlate(window[1], residual[0])
    crossed = jnp.stack([real_part, imag_part])
    trace_rows, window_len = crossed.shape[-2:]
    leading = crossed.shape[:-2]
    flattened = crossed.reshape(leading + (trace_rows * window_len,))
    flattened = jnp.concatenate([flattened, jnp.zeros(leading + (trace_rows,), jnp.float32)], -1)
    column_sums = jnp.sum(flattened.reshape(leading + (trace_rows, window_len + 1)), axis=-2)
    return column_sums[..., 1:tap_count + 1][..., ::-1]


def reference(recorded, multiples):
    half_taps = TAPS // 2
    tile_rows = NX // N_TRACE
    window_len = tile_rows + TAPS
    padded = jnp.pad(multiples, ((0, 0), (0, 0), (0, 0), (half_taps, half_taps)))
    tiles_all = jnp.stack([padded[..., tile_index * tile_rows: tile_index * tile_rows + window_len] for tile_index in range(N_TRACE)])
    tiles_all = tiles_all.reshape(N_TRACE, SHOTS, 2, NB, FB, window_len)
    weight = 0.5 * FB * NX

    def forward(shaping):
        result = lax.map(lambda tile: lax.map(lambda paired: forward_one(paired[0], paired[1]), (tile, shaping)), tiles_all)
        return jnp.moveaxis(result, 0, 4).reshape(SHOTS, 2, NF, NX)

    def adjoint(residual):
        pieces = jnp.moveaxis(residual.reshape(SHOTS, 2, NB, FB, N_TRACE, tile_rows), 4, 0)
        result = lax.map(lambda paired: lax.map(lambda inner_pair: adjoint_one(inner_pair[0], inner_pair[1], TAPS), paired), (tiles_all, pieces))
        return jnp.sum(result, axis=0)

    def bending(vector):
        edge_pad = jnp.pad(vector, ((0, 0), (0, 0), (1, 1), (0, 0)))
        return 2.0 * vector - edge_pad[:, :, :-2] - edge_pad[:, :, 2:]

    def inner_sum(left, right):
        return jnp.sum(left * right, axis=(1, 2, 3))

    shaping = jnp.zeros((SHOTS, 2, NB, TAPS), jnp.float32)
    bent_sum = jnp.zeros((SHOTS, 2, NB, TAPS), jnp.float32)
    residual = recorded
    direction = shaping
    norm_now = jnp.ones((SHOTS,), jnp.float32)
    for iteration in range(ITERS):
        gradient = adjoint(residual) - bent_sum
        norm_next = inner_sum(gradient, gradient)
        if iteration == 0:
            direction = gradient
        else:
            direction = gradient + (norm_next / norm_now)[:, None, None, None] * direction
        norm_now = norm_next
        applied = forward(direction)
        smooth = weight * bending(direction)
        energy = inner_sum(applied, applied) + inner_sum(direction, smooth)
        step_len = (norm_now / energy)[:, None, None, None]
        shaping = shaping + step_len * direction
        residual = residual - step_len * applied
        bent_sum = bent_sum + step_len * smooth
    return residual, shaping
```

```python
import functools

import jax
import jax.numpy as jnp
import numpy as np
from jax import lax
from jax.experimental import pallas as pl
from jax.experimental.pallas import tpu as pltpu
from jax.sharding import PartitionSpec as P

FB = 64
TAPS = 64
ITERS = 3
HALF = TAPS // 2
LANES = 128
POINTS = 2 * LANES
F32 = jnp.float32
BF16 = jnp.bfloat16
MESH = pl.DeviceIdType.MESH


def lanes_of(shape):
    return lax.broadcasted_iota(jnp.int32, shape, len(shape) - 1)


def turn(value, shift):
    shift = shift % LANES
    return value if shift == 0 else pltpu.roll(value, shift, 1)


def split(value):
    high = value.astype(BF16)
    return high, (value - high.astype(F32)).astype(BF16)


def waves(positions):
    phase = (2 * np.pi / POINTS) * np.outer(np.asarray(positions), np.arange(LANES) + 0.5)
    return np.cos(phase), np.sin(phase)


def both_waves(positions):
    return np.concatenate(waves(positions), 1)


def halves(table):
    high = table.astype(np.float32).astype(BF16)
    return high, (table - high.astype(np.float64)).astype(np.float32).astype(BF16)


def fit_tables():
    high, low = halves(both_waves(np.arange(LANES)))
    tail_high, tail_low = halves(both_waves(LANES + np.arange(TAPS)))
    tail = np.concatenate([tail_high, tail_high, tail_low, np.zeros_like(tail_low)], 0)
    lag_cos, lag_sin = waves(np.arange(TAPS))
    none = np.zeros((LANES, TAPS))
    lags = np.block([[lag_cos.T, none], [none, 2.0 * lag_sin.T]]) / LANES
    right = both_waves(-1 - np.arange(TAPS)).T
    none = np.zeros_like(right)
    sides = np.block([[right, none], [none, right]]) / LANES
    return (
        np.concatenate([high, high], 0),
        low,
        tail,
        lags.astype(np.float32),
        sides.astype(np.float32),
    )


def forward_tables():
    taps = both_waves(np.arange(TAPS))
    none = np.zeros_like(taps)
    high, low = halves(np.block([[taps, none], [none, taps]]))
    back = halves(both_waves(TAPS + np.arange(LANES)).T / LANES)
    return np.concatenate([high, high], 0), low, np.concatenate(back, 1)


def three(pair):
    (rh, rl), (ih, il) = pair
    return jnp.concatenate([rh, ih, rh, ih, rl, il], 0)


def three_re(pair):
    (rh, rl), (ih, il) = pair
    return jnp.concatenate([rh, ih, rl, il, rh, ih], 0)


def three_im(pair):
    (rh, rl), (ih, il) = pair
    return jnp.concatenate([ih, -rh, il, -rl, ih, -rh], 0)


def over_first(left, right):
    return lax.dot_general(left, right, (((0,), (0,)), ((), ())), preferred_element_type=F32)


def product(left, right):
    return jnp.dot(left, right, preferred_element_type=F32)


def exact(left, right):
    return jnp.dot(left, right, precision=lax.Precision.HIGHEST, preferred_element_type=F32)


def mirror(total):
    rows = lax.broadcasted_iota(jnp.int32, (LANES, LANES), 0)
    return (rows + lanes_of((LANES, LANES)) == total).astype(F32)


def total_of(value):
    return jnp.sum(jnp.sum(value, axis=1, keepdims=True), axis=0, keepdims=True)


def column_sum(value):
    return jnp.sum(value, axis=0, keepdims=True)


def pack_edges(m, edge, s):
    freq_rows = m.shape[2]
    groups = LANES // HALF
    rows = freq_rows // groups
    lane = lanes_of((rows, LANES))
    for part in range(2):
        for side in range(2):
            packed = None
            for g in range(groups):
                shift = HALF * g + HALF if side == 0 else HALF * g
                value = turn(m[s, part, g * rows : (g + 1) * rows, :], shift)
                packed = value if packed is None else jnp.where(lane >= HALF * g, value, packed)
            edge[side, s, part] = packed


def corners(m, corner, s, keep):
    for b in range(m.shape[2] // FB):
        ends = [split(turn(m[s, part, b * FB : (b + 1) * FB, :], HALF)) for part in range(2)]
        edge = over_first(three(ends)[:, :TAPS], jnp.concatenate([three_re(ends), three_im(ends)], 1))
        real, imag = edge[:, :LANES], turn(edge[:, LANES:], TAPS)
        lane = lanes_of((HALF, LANES))
        value = jnp.where(
            lane < HALF,
            real[:HALF],
            jnp.where(lane < TAPS, real[HALF:], jnp.where(lane < TAPS + HALF, imag[:HALF], imag[HALF:])),
        )
        corner[s, :, b, :] = jnp.where(keep, value, 0.0)


def statistics(m, rec, halo, spec, sums, wide, low, tail, s):
    freq_rows = m.shape[2]
    group_rows = freq_rows * HALF // LANES
    lane = lanes_of((FB, LANES))
    for b in range(freq_rows // FB):
        rows = slice(b * FB, (b + 1) * FB)
        group, first = (b * FB) // group_rows, (b * FB) % group_rows
        near = slice(first, first + FB)
        starts, tails = [], []
        for part in range(2):
            turned = turn(m[s, part, rows, :], HALF)
            left = turn(halo[0, s, part, near, :], -HALF * group)
            right = turn(halo[1, s, part, near, :], HALF - HALF * group)
            starts.append(jnp.where(lane < HALF, left, turned))
            tails.append(jnp.where(lane < HALF, turned, right))
        high, rest = split(jnp.concatenate(starts + [rec[s, 0, rows, :], rec[s, 1, rows, :]], 0))
        main = product(jnp.concatenate([high, rest], 1), wide[...]) + product(high, low[...])
        ends = jnp.concatenate(tails, 0)
        top = ends.astype(BF16)
        mixed = jnp.where(
            lanes_of(ends.shape) < TAPS, ends, turn(ends - top.astype(F32), TAPS)
        ).astype(BF16)
        last = product(jnp.concatenate([mixed, top], 1), tail[...])

        def parts(value, first):
            return value[first : first + FB, :LANES], value[first : first + FB, LANES:]

        s_all = parts(main, 0) + parts(main, FB)
        t_all = parts(last, 0) + parts(last, FB)
        r_ac, r_as, r_bc, r_bs = parts(main, 2 * FB) + parts(main, 3 * FB)
        w_all = [x + y for x, y in zip(s_all, t_all)]
        for i in range(4):
            spec[s, i, rows, :] = w_all[i]
        w_ac, w_as, w_bc, w_bs = w_all
        t_ac, t_as, t_bc, t_bs = t_all
        power = sum(x * (w + t) for x, w, t in zip(s_all, w_all, t_all))
        cross = (w_ac * w_bs - w_as * w_bc) - (t_ac * t_bs - t_as * t_bc)
        found = [
            power,
            cross,
            w_ac * r_ac + w_as * r_as + w_bc * r_bc + w_bs * r_bs,
            w_ac * r_as - w_as * r_ac + w_bc * r_bs - w_bs * r_bc,
            w_ac * r_bc + w_as * r_bs - w_bc * r_ac - w_bs * r_as,
            w_ac * r_bs - w_as * r_bc - w_bc * r_as + w_bs * r_ac,
        ]
        for i in range(6):
            sums[i, s, b : b + 1, :] = column_sum(found[i])


def prepare_corners(corner, matrix, slot):
    blocks = corner.shape[0] * corner.shape[3]

    def row(r):
        return corner[:, slot, r, :, :].reshape(blocks, LANES)

    lane = lanes_of((blocks, LANES))
    place = lane % TAPS
    carry_right = place < HALF - 1
    carry_left = place > HALF
    in_right = place < HALF
    right = None
    for i in reversed(range(HALF)):
        value = jnp.where(in_right, row(i), 0.0)
        if right is not None:
            value = value + jnp.where(carry_right, turn(right, -1), 0.0)
        right = value
        if i >= 1:
            matrix[i - 1] = jnp.where(carry_right, turn(value, -1), 0.0)
    matrix[HALF - 1] = jnp.zeros((blocks, LANES), F32)
    last = None
    for i in range(HALF):
        value = jnp.where(in_right, 0.0, row(i))
        if i:
            value = value + jnp.where(carry_left, turn(last, 1), 0.0)
        last = value
        matrix[HALF + i] = value
    matrix[TAPS] = right


def solve(weight, lag, gradient, matrix):
    blocks = lag.shape[0]
    lane = lanes_of((blocks, LANES))
    is_real = lane < TAPS
    right = matrix[TAPS]
    lag_real = jnp.where(is_real, lag, 0.0) + jnp.where(lane < HALF, right, 0.0)
    lag_imag = jnp.where(is_real, turn(lag, TAPS), 0.0) + jnp.where(lane < HALF, turn(right, TAPS), 0.0)
    back = mirror(LANES)
    toep_real = jnp.where(is_real, lag_real, exact(lag_real, back))
    toep_imag = jnp.where(is_real, -lag_imag, exact(lag_imag, back))
    for t in range(TAPS):
        toep = jnp.where(is_real, turn(toep_real, t), turn(toep_imag, TAPS + t))
        matrix[t] = toep - jnp.where(is_real, matrix[t], -matrix[t])

    filters = jnp.zeros((blocks, LANES), F32)
    direction = norm_now = None
    none = jnp.zeros((1, LANES), F32)
    for iteration in range(ITERS):
        norm_next = total_of(gradient * gradient)
        if iteration == 0:
            direction = gradient
        else:
            direction = gradient + (norm_next / norm_now) * direction
        norm_now = norm_next
        by_real = jnp.zeros((blocks, LANES), F32)
        by_imag = jnp.zeros((blocks, LANES), F32)
        for t in range(TAPS):
            by_real = by_real + direction[:, t : t + 1] * matrix[t]
            by_imag = by_imag + direction[:, TAPS + t : TAPS + t + 1] * matrix[t]
        by_imag = turn(by_imag, TAPS)
        normal = by_real + jnp.where(is_real, -by_imag, by_imag)
        before = jnp.concatenate([none, direction[:-1]], 0)
        after = jnp.concatenate([direction[1:], none], 0)
        normal = normal + weight * (2.0 * direction - before - after)
        step_len = norm_now / total_of(direction * normal)
        filters = filters + step_len * direction
        gradient = gradient - step_len * normal
    rows = lax.broadcasted_iota(jnp.int32, (LANES, LANES), 0)
    columns = lanes_of((LANES, LANES))
    flip = (rows + columns == jnp.where(columns < TAPS, TAPS - 1, 3 * TAPS - 1)).astype(F32)
    return exact(filters, flip)


def fit_kernel(
    weight,
    trace_count,
    freq_count,
    per_device,
    relay_at,
    m_any,
    rec_any,
    wide,
    low,
    tail,
    lags,
    sides,
    taps_out,
    spec_any,
    m,
    rec,
    edge,
    halo,
    spec,
    sums,
    corner,
    corner_in,
    corner_all,
    stats,
    stats_in,
    stats_all,
    taps,
    solved,
    matrix,
    m_sem,
    rec_sem,
    spec_sem,
    edge_send,
    halo_sem,
    corner_send,
    corner_sem,
    relay_send,
    relay_sem,
    stats_send,
    stats_sem,
    gather_send,
    gather_sem,
    taps_send,
    taps_sem,
):
    shots = m.shape[0]
    blocks = m.shape[2] // FB
    owners = -(-shots // per_device)
    last = trace_count - 1
    me = lax.axis_index("trace")
    layer = lax.axis_index("freq")
    at_edge = (me == 0) | (me == last)
    owns = me < owners

    def remote(source, target, send, arrive, **where):
        return pltpu.make_async_remote_copy(
            src_ref=source,
            dst_ref=target,
            send_sem=send,
            recv_sem=arrive,
            device_id=where,
            device_id_type=MESH,
        )

    def load(source, target, sem, s):
        return pltpu.make_async_copy(source.at[s], target.at[s], sem.at[s])

    for s in range(shots):
        load(m_any, m, m_sem, s).start()
    for s in range(shots):
        load(rec_any, rec, rec_sem, s).start()

    barrier = pltpu.get_barrier_semaphore()
    for o in range(1, trace_count):
        pl.semaphore_signal(
            barrier, inc=1, device_id={"trace": lax.rem(me + o, trace_count)}, device_id_type=MESH
        )
    for o in range(1, freq_count):
        pl.semaphore_signal(
            barrier, inc=1, device_id={"freq": lax.rem(layer + o, freq_count)}, device_id_type=MESH
        )
    pl.semaphore_wait(barrier, trace_count + freq_count - 2)

    def halo_copy(side, s):
        other = jnp.minimum(me + 1, last) if side == 0 else jnp.maximum(me - 1, 0)
        return remote(
            edge.at[side, s], halo.at[side, s], edge_send.at[side, s], halo_sem.at[side, s], trace=other
        )

    sends = (me < last, me > 0)
    receives = (me > 0, me < last)

    @pl.when(me == 0)
    def _():
        halo[0] = jnp.zeros(halo.shape[1:], F32)

    @pl.when(me == last)
    def _():
        halo[1] = jnp.zeros(halo.shape[1:], F32)

    def send_edges(s, carry):
        load(m_any, m, m_sem, s).wait()
        pack_edges(m, edge, s)
        for side in range(2):

            @pl.when(sends[side])
            def _():
                halo_copy(side, s).start()

        return carry

    lax.fori_loop(0, shots, send_edges, 0)

    def corner_copy(end, s, owner, slot):
        return remote(
            corner.at[s], corner_in.at[end, slot], corner_send.at[s], corner_sem.at[end, slot], trace=owner
        )

    place = lanes_of((HALF, LANES)) % TAPS < HALF
    keep = (place & (me == last)) | (jnp.logical_not(place) & (me == 0))

    @pl.when(at_edge)
    def _():
        def fill(s, carry):
            corners(m, corner, s, keep)
            owner, slot = s // per_device, s % per_device
            for end, where in ((0, 0), (1, last)):

                @pl.when((me == where) & (owner != where))
                def _():
                    corner_copy(end, s, owner, slot).start()

                @pl.when((me == where) & (owner == where))
                def _():
                    corner_in[end, slot] = corner[s]

            return carry

        lax.fori_loop(0, shots, fill, 0)

    def relay_copy(o):
        return remote(
            corner_all.at[layer],
            corner_all.at[layer],
            relay_send.at[o],
            relay_sem.at[layer],
            freq=lax.rem(layer + o, freq_count),
        )

    def relay():
        for slot in range(per_device):
            for end, where in ((0, 0), (1, last)):

                @pl.when(me != where)
                def _():
                    corner_copy(end, 0, me, slot).wait_recv()

            corner_all[layer, slot] = corner_in[0, slot] + corner_in[1, slot]
        for o in range(1, freq_count):
            relay_copy(o).start()

    def measure(s, carry):
        load(rec_any, rec, rec_sem, s).wait()
        for side in range(2):

            @pl.when(receives[side])
            def _():
                halo_copy(side, s).wait_recv()

        statistics(m, rec, halo, spec, sums, wide, low, tail, s)
        pltpu.make_async_copy(spec.at[s], spec_any.at[s], spec_sem.at[s]).start()

        @pl.when((s == relay_at) & owns)
        def _():
            relay()

        return carry

    lax.fori_loop(0, shots, measure, 0)

    def flat(i):
        return sums[i].reshape(shots * blocks, LANES)

    lag = exact(jnp.concatenate([flat(0), flat(1)], 1), lags[...])
    side = exact(jnp.concatenate([flat(i) for i in range(2, 6)], 1), sides[...])
    stats[:, 0] = lag.reshape(shots, blocks, LANES)
    stats[:, 1] = side.reshape(shots, blocks, LANES)

    def stats_copy(s):
        return remote(
            stats.at[s],
            stats_in.at[me, s % per_device],
            stats_send.at[s],
            stats_sem.at[me, s % per_device],
            trace=s // per_device,
        )

    for s in range(shots):

        @pl.when(me != s // per_device)
        def _():
            stats_copy(s).start()

    def gather_copy(o):
        return remote(
            stats_all.at[layer],
            stats_all.at[layer],
            gather_send.at[o],
            gather_sem.at[layer],
            freq=lax.rem(layer + o, freq_count),
        )

    def taps_copy(o):
        own = pl.ds(me * per_device, per_device)
        return remote(
            taps.at[own], taps.at[own], taps_send.at[o], taps_sem.at[me], trace=lax.rem(me + o, trace_count)
        )

    def solve_own():
        for o in range(1, freq_count):
            other = lax.rem(layer + o, freq_count)
            remote(
                corner_all.at[other], corner_all.at[other], relay_send.at[o], relay_sem.at[other], freq=other
            ).wait_recv()
        for slot in range(per_device):
            prepare_corners(corner_all, matrix.at[slot], slot)
        for slot in range(per_device):
            whole = stats[me * per_device + slot]
            for o in range(1, trace_count):
                other = lax.rem(me + o, trace_count)
                remote(
                    stats.at[slot],
                    stats_in.at[other, slot],
                    stats_send.at[slot],
                    stats_sem.at[other, slot],
                    trace=other,
                ).wait_recv()
                whole = whole + stats_in[other, slot]
            stats_all[layer, slot] = whole
        for o in range(1, freq_count):
            gather_copy(o).start()
        for o in range(1, freq_count):
            other = lax.rem(layer + o, freq_count)
            remote(
                stats_all.at[other], stats_all.at[other], gather_send.at[o], gather_sem.at[other], freq=other
            ).wait_recv()
        for slot in range(per_device):
            lag_rows, gradient = [
                stats_all[:, slot, i].reshape(freq_count * blocks, LANES) for i in range(2)
            ]
            found = solve(weight, lag_rows, gradient, matrix.at[slot])
            solved[...] = found.reshape(freq_count, blocks, LANES)
            taps[me * per_device + slot] = solved[layer]
        for o in range(1, trace_count):
            taps_copy(o).start()

    if owners == trace_count:
        solve_own()
    else:
        pl.when(owns)(solve_own)

    for o in range(1, trace_count):
        other = lax.rem(me + o, trace_count)

        def arrived():
            own = pl.ds(other * per_device, per_device)
            remote(taps.at[own], taps.at[own], taps_send.at[o], taps_sem.at[other], trace=other).wait_recv()

        if owners == trace_count:
            arrived()
        else:
            pl.when(other < owners)(arrived)
    taps_out[...] = taps[:shots]

    def drain(s, carry):
        for side in range(2):

            @pl.when(sends[side])
            def _():
                halo_copy(side, s).wait_send()

        owner = s // per_device
        for end, where in ((0, 0), (1, last)):

            @pl.when((me == where) & (owner != where))
            def _():
                corner_copy(end, s, owner, s % per_device).wait_send()

        @pl.when(me != owner)
        def _():
            stats_copy(s).wait_send()

        pltpu.make_async_copy(spec.at[s], spec_any.at[s], spec_sem.at[s]).wait()
        return carry

    lax.fori_loop(0, shots, drain, 0)

    def drain_own():
        for o in range(1, freq_count):
            relay_copy(o).wait_send()
            gather_copy(o).wait_send()
        for o in range(1, trace_count):
            taps_copy(o).wait_send()

    if owners == trace_count:
        drain_own()
    else:
        pl.when(owns)(drain_own)


def forward_kernel(taps_ref, wide, low, back, spec_ref, rec_ref, out_ref, filters_ref, shaped):
    shots, blocks, _ = taps_ref.shape
    s = pl.program_id(0)

    @pl.when(s == 0)
    def _():
        high, rest = split(taps_ref[...].reshape(shots * blocks, LANES))
        value = product(jnp.concatenate([high, rest], 1), wide[...]) + product(high, low[...])
        shaped[...] = value.reshape(shots, blocks, 4 * LANES)

    own = taps_ref[s]
    filters_ref[0, 0] = own[:, :TAPS]
    filters_ref[0, 1] = turn(own, TAPS)[:, :TAPS]
    for b in range(blocks):
        rows = slice(b * FB, (b + 1) * FB)
        w_ac, w_as, w_bc, w_bs = [spec_ref[0, i, rows, :] for i in range(4)]
        h_ac, h_as, h_bc, h_bs = [shaped[s, b : b + 1, i * LANES : (i + 1) * LANES] for i in range(4)]
        y_ac = h_ac * w_ac - h_as * w_as - h_bc * w_bc + h_bs * w_bs
        y_as = h_ac * w_as + h_as * w_ac - h_bc * w_bs - h_bs * w_bc
        y_bc = h_ac * w_bc - h_as * w_bs + h_bc * w_ac - h_bs * w_as
        y_bs = h_ac * w_bs + h_as * w_bc + h_bc * w_as + h_bs * w_ac
        both = jnp.concatenate(
            [jnp.concatenate([y_ac, y_as], 1), jnp.concatenate([y_bc, y_bs], 1)], 0
        )
        value = product(jnp.concatenate(split(both), 0), back[...])
        value = value[: 2 * FB] + value[2 * FB :]
        applied = value[:, :LANES] + value[:, LANES:]
        out_ref[0, 0, rows, :] = rec_ref[0, 0, rows, :] - applied[:FB]
        out_ref[0, 1, rows, :] = rec_ref[0, 1, rows, :] - applied[FB:]


def body(recorded, multiples):
    shots, parts, freq_rows, trace_rows = multiples.shape
    blocks = freq_rows // FB
    trace_count, freq_count = lax.axis_size("trace"), lax.axis_size("freq")
    weight = 0.5 * FB * trace_rows * trace_count
    per_device = -(-shots // trace_count)
    owners = -(-shots // per_device)
    pack_rows = freq_rows * HALF // LANES
    relay_at = min(2, shots - 1)

    tables = fit_tables()
    field = (shots, parts, freq_rows, trace_rows)
    dma = pltpu.SemaphoreType.DMA
    vmem = pl.BlockSpec(memory_space=pltpu.VMEM)
    anywhere = pl.BlockSpec(memory_space=pl.ANY)
    taps, spec = pl.pallas_call(
        functools.partial(fit_kernel, weight, trace_count, freq_count, per_device, relay_at),
        in_specs=[anywhere, anywhere] + [vmem] * len(tables),
        out_specs=[vmem, anywhere],
        out_shape=[
            jax.ShapeDtypeStruct((shots, blocks, LANES), F32),
            jax.ShapeDtypeStruct((shots, 4, freq_rows, LANES), F32),
        ],
        scratch_shapes=[
            pltpu.VMEM(field, F32),
            pltpu.VMEM(field, F32),
            pltpu.VMEM((2, shots, parts, pack_rows, LANES), F32),
            pltpu.VMEM((2, shots, parts, pack_rows, LANES), F32),
            pltpu.VMEM((shots, 4, freq_rows, LANES), F32),
            pltpu.VMEM((6, shots, blocks, LANES), F32),
            pltpu.VMEM((shots, HALF, blocks, LANES), F32),
            pltpu.VMEM((2, per_device, HALF, blocks, LANES), F32),
            pltpu.VMEM((freq_count, per_device, HALF, blocks, LANES), F32),
            pltpu.VMEM((shots, 2, blocks, LANES), F32),
            pltpu.VMEM((trace_count, per_device, 2, blocks, LANES), F32),
            pltpu.VMEM((freq_count, per_device, 2, blocks, LANES), F32),
            pltpu.VMEM((owners * per_device, blocks, LANES), F32),
            pltpu.VMEM((freq_count, blocks, LANES), F32),
            pltpu.VMEM((per_device, TAPS + 1, freq_count * blocks, LANES), F32),
            dma((shots,)),
            dma((shots,)),
            dma((shots,)),
            dma((2, shots)),
            dma((2, shots)),
            dma((shots,)),
            dma((2, per_device)),
            dma((freq_count,)),
            dma((freq_count,)),
            dma((shots,)),
            dma((trace_count, per_device)),
            dma((freq_count,)),
            dma((freq_count,)),
            dma((trace_count,)),
            dma((trace_count,)),
        ],
        compiler_params=pltpu.CompilerParams(
            collective_id=0, has_side_effects=True, vmem_limit_bytes=56 * 1024 * 1024
        ),
        name="fit",
    )(multiples, recorded, *[jnp.asarray(table) for table in tables])

    tables = forward_tables()
    block = pl.BlockSpec((1, parts, freq_rows, trace_rows), lambda s: (s, 0, 0, 0))
    fixed = [pl.BlockSpec(table.shape, lambda s: (0, 0)) for table in tables]
    return pl.pallas_call(
        forward_kernel,
        grid=(shots,),
        in_specs=[
            pl.BlockSpec((shots, blocks, LANES), lambda s: (0, 0, 0)),
            *fixed,
            pl.BlockSpec((1, 4, freq_rows, LANES), lambda s: (s, 0, 0, 0)),
            block,
        ],
        out_specs=[block, pl.BlockSpec((1, parts, blocks, TAPS), lambda s: (s, 0, 0, 0))],
        out_shape=[
            jax.ShapeDtypeStruct(field, F32),
            jax.ShapeDtypeStruct((shots, parts, blocks, TAPS), F32),
        ],
        scratch_shapes=[pltpu.VMEM((shots, blocks, 4 * LANES), F32)],
        name="forward",
    )(taps, *[jnp.asarray(table) for table in tables], spec, recorded)


def solution(mesh):
    spec = P(None, None, "freq", "trace")
    return jax.shard_map(
        body,
        mesh=mesh,
        in_specs=(spec, spec),
        out_specs=(spec, P(None, None, "freq", None)),
        check_vma=False,
    )
```

```python
import functools

import jax
import jax.numpy as jnp
import numpy as np
from jax import lax
from jax.experimental import pallas as pl
from jax.experimental.pallas import tpu as pltpu
from jax.sharding import PartitionSpec as P

FB = 64
TAPS = 64
ITERS = 3
HALF = TAPS // 2
LANES = 128
POINTS = 2 * LANES
F32 = jnp.float32
BF16 = jnp.bfloat16
MESH = pl.DeviceIdType.MESH


def lanes_of(shape):
    return lax.broadcasted_iota(jnp.int32, shape, len(shape) - 1)


def turn(value, shift):
    shift = shift % LANES
    return value if shift == 0 else pltpu.roll(value, shift, 1)


def split(value):
    high = value.astype(BF16)
    return high, (value - high.astype(F32)).astype(BF16)


def waves(positions):
    phase = (2 * np.pi / POINTS) * np.outer(np.asarray(positions), np.arange(LANES) + 0.5)
    return np.cos(phase), np.sin(phase)


def both_waves(positions):
    return np.concatenate(waves(positions), 1)


def halves(table):
    high = table.astype(np.float32).astype(BF16)
    return high, (table - high.astype(np.float64)).astype(np.float32).astype(BF16)


def all_tables():
    high, low = halves(both_waves(np.arange(LANES)))
    tail_high, tail_low = halves(both_waves(LANES + np.arange(TAPS)))
    lag = np.where(np.arange(LANES) < TAPS, np.arange(LANES), LANES - np.arange(LANES))
    used = (np.arange(LANES) != TAPS) / LANES
    sign = np.where(np.arange(LANES) < TAPS, -2.0, 2.0)
    lag_cos, lag_sin = waves(lag)
    right = both_waves(-1 - np.arange(TAPS)).T / LANES
    none = np.zeros_like(right)
    shape_high, shape_low = halves(both_waves(np.arange(TAPS)))
    parts = dict(
        wide=[high, high],
        low=[low],
        tail=[tail_high, tail_high, tail_low, np.zeros_like(tail_low)],
        power=[np.concatenate(halves(lag_cos.T * used), 1)],
        cross=[np.concatenate(halves(lag_sin.T * (sign * used)), 1)],
        sides=[np.concatenate(halves(np.block([[right, none], [none, right]])), 1)],
        shape=[shape_high, shape_high, shape_low, np.zeros_like(shape_low)],
        back=[np.concatenate(halves(both_waves(TAPS + np.arange(LANES)).T / LANES), 1)],
    )
    parts = {name: np.concatenate(part, 0) for name, part in parts.items()}
    runs, start = {}, 0
    for name, part in parts.items():
        runs[name] = slice(start, start + part.shape[0])
        start += part.shape[0]
    return np.concatenate(list(parts.values()), 0), runs


def over_first(left, right):
    return lax.dot_general(left, right, (((0,), (0,)), ((), ())), preferred_element_type=F32)


def product(left, right):
    return jnp.dot(left, right, preferred_element_type=F32)


def exact(left, right):
    return jnp.dot(left, right, precision=lax.Precision.HIGHEST, preferred_element_type=F32)


def mirror(total):
    rows = lax.broadcasted_iota(jnp.int32, (LANES, LANES), 0)
    return (rows + lanes_of((LANES, LANES)) == total).astype(F32)


def total_of(value):
    return jnp.sum(jnp.sum(value, axis=1, keepdims=True), axis=0, keepdims=True)


def column_sum(value):
    return jnp.sum(value, axis=0, keepdims=True)


def pack_edges(m, edge, s):
    freq_rows = m.shape[2]
    groups = LANES // HALF
    rows = freq_rows // groups
    lane = lanes_of((rows, LANES))
    for part in range(2):
        for side in range(2):
            packed = None
            for g in range(groups):
                shift = HALF * g + HALF if side == 0 else HALF * g
                value = turn(m[s, part, g * rows : (g + 1) * rows, :], shift)
                packed = value if packed is None else jnp.where(lane >= HALF * g, value, packed)
            edge[side, s, part] = packed


def corners(m, ends, corner, s, at_last):
    freq_rows = m.shape[2]
    wide = (freq_rows, LANES)
    lane = lanes_of(wide)
    real = pltpu.roll(m[s, 0], jnp.where(at_last, HALF, 0), 1)
    imag = pltpu.roll(m[s, 1], jnp.where(at_last, 2 * HALF, HALF), 1)
    both = jnp.where(lane < HALF, real, imag)
    rest = both - both.astype(BF16).astype(F32)
    ends[...] = jnp.where(lane < TAPS, both, turn(rest, TAPS)).astype(BF16)
    lane = lanes_of((HALF, LANES))
    for b in range(freq_rows // FB):
        part = ends[b * FB : (b + 1) * FB, :]
        gram = over_first(part, part)
        gram = gram[:TAPS] + gram[TAPS:]
        gram = gram + turn(gram, TAPS)
        one, two = gram[:HALF], turn(gram[HALF:], HALF)
        value = jnp.where(lane % TAPS < HALF, one + two, one - two)
        corner[s, :, b, :] = jnp.where(
            lane[: HALF // 2] < TAPS, value[: HALF // 2], value[HALF // 2 :]
        )


def joined_corners(left, right):
    shape = left.shape
    lane = lanes_of(shape)

    def moved(value, shift):
        return pltpu.roll(value, shift % LANES, 2)

    def pick(*values):
        result = values[0]
        for i in range(1, 4):
            result = jnp.where(lane >= i * HALF, values[i], result)
        return result

    first = pick(right, moved(left, HALF), moved(right, HALF), moved(left, TAPS))
    second = pick(moved(right, TAPS), moved(left, -HALF), moved(right, -HALF), left)
    value = jnp.concatenate([first, second], 0)
    place = lanes_of(value.shape) % TAPS
    step = 1
    while step < HALF:
        none = jnp.zeros((step,) + shape[1:], F32)
        later = jnp.concatenate([moved(value[step:], -step), none], 0)
        sooner = jnp.concatenate([none, moved(value[:-step], step)], 0)
        value = value + jnp.where(
            place < HALF - step, later, jnp.where(place >= HALF + step, sooner, 0.0)
        )
        step *= 2
    return value


def fourfold(value, table):
    count = value.shape[0]
    both = product(jnp.concatenate(split(value), 0), table)
    both = both[:count] + both[count:]
    return both[:, :LANES] + both[:, LANES:]


def threefold(value, table):
    top = value.astype(BF16)
    rest = turn(value - top.astype(F32), TAPS)
    mixed = jnp.where(lanes_of(value.shape) < TAPS, value, rest).astype(BF16)
    return product(jnp.concatenate([mixed, top], 1), table)


def statistics(m, rec, halo, spec, sums, table, s):
    freq_rows = m.shape[2]
    group_rows = freq_rows * HALF // LANES
    lane = lanes_of((FB, LANES))
    for b in range(freq_rows // FB):
        rows = slice(b * FB, (b + 1) * FB)
        group, first = (b * FB) // group_rows, (b * FB) % group_rows
        near = slice(first, first + FB)
        starts, tails = [], []
        for part in range(2):
            turned = turn(m[s, part, rows, :], HALF)
            left = turn(halo[0, s, part, near, :], -HALF * group)
            right = turn(halo[1, s, part, near, :], HALF - HALF * group)
            starts.append(jnp.where(lane < HALF, left, turned))
            tails.append(jnp.where(lane < HALF, turned, right))
        high, rest = split(jnp.concatenate(starts + [rec[s, 0, rows, :], rec[s, 1, rows, :]], 0))
        main = product(jnp.concatenate([high, rest], 1), table("wide")) + product(high, table("low"))
        last = threefold(jnp.concatenate(tails, 0), table("tail"))

        def parts(value, first):
            return value[first : first + FB, :LANES], value[first : first + FB, LANES:]

        s_all = parts(main, 0) + parts(main, FB)
        t_all = parts(last, 0) + parts(last, FB)
        r_ac, r_as, r_bc, r_bs = parts(main, 2 * FB) + parts(main, 3 * FB)
        w_all = [x + y for x, y in zip(s_all, t_all)]
        for i in range(4):
            spec[s, i, rows, :] = w_all[i]
        w_ac, w_as, w_bc, w_bs = w_all
        t_ac, t_as, t_bc, t_bs = t_all
        power = sum(x * (w + t) for x, w, t in zip(s_all, w_all, t_all))
        cross = (w_ac * w_bs - w_as * w_bc) - (t_ac * t_bs - t_as * t_bc)
        found = [
            power,
            cross,
            w_ac * r_ac + w_as * r_as + w_bc * r_bc + w_bs * r_bs,
            w_ac * r_as - w_as * r_ac + w_bc * r_bs - w_bs * r_bc,
            w_ac * r_bc + w_as * r_bs - w_bc * r_ac - w_bs * r_as,
            w_ac * r_bs - w_as * r_bc - w_bc * r_as + w_bs * r_ac,
        ]
        for i in range(6):
            sums[i, b : b + 1, :] = column_sum(found[i])


def prepare_corners(corner, matrix):
    blocks = corner.shape[0] * corner.shape[2]

    def row(r):
        return corner[:, r, :, :].reshape(blocks, LANES)

    lane = lanes_of((blocks, LANES))
    place = lane % TAPS
    is_real = lane < TAPS
    for i in range(HALF):
        value = row(i)
        if i:
            moved = jnp.where(place < HALF - 1, turn(value, -1), 0.0)
            matrix[i - 1] = jnp.where(is_real, -moved, moved)
        value = jnp.where(place < HALF, 0.0, value)
        matrix[HALF + i] = jnp.where(is_real, -value, value)
    matrix[HALF - 1] = jnp.zeros((blocks, LANES), F32)
    right = jnp.where(place < HALF, row(0), 0.0)
    add_real = jnp.where(lane < HALF, right, 0.0)
    add_imag = jnp.where(lane < HALF, turn(right, TAPS), 0.0)
    back = mirror(LANES)
    matrix[TAPS] = jnp.where(is_real, add_real, exact(add_real, back))
    matrix[TAPS + 1] = jnp.where(is_real, -add_imag, exact(add_imag, back))


def solve(weight, toep_real, toep_imag, gradient, matrix):
    blocks = gradient.shape[0]
    lane = lanes_of((blocks, LANES))
    is_real = lane < TAPS
    toep_real = toep_real + matrix[TAPS]
    toep_imag = toep_imag + matrix[TAPS + 1]
    for t in range(TAPS):
        matrix[t] += jnp.where(is_real, turn(toep_real, t), turn(toep_imag, TAPS + t))

    filters = jnp.zeros((blocks, LANES), F32)
    direction = norm_now = None
    none = jnp.zeros((1, LANES), F32)
    for iteration in range(ITERS):
        norm_next = total_of(gradient * gradient)
        if iteration == 0:
            direction = gradient
        else:
            direction = gradient + (norm_next / norm_now) * direction
        norm_now = norm_next
        by_real = jnp.zeros((blocks, LANES), F32)
        by_imag = jnp.zeros((blocks, LANES), F32)
        for t in range(TAPS):
            by_real = by_real + direction[:, t : t + 1] * matrix[t]
            by_imag = by_imag + direction[:, TAPS + t : TAPS + t + 1] * matrix[t]
        by_imag = turn(by_imag, TAPS)
        normal = by_real + jnp.where(is_real, -by_imag, by_imag)
        before = jnp.concatenate([none, direction[:-1]], 0)
        after = jnp.concatenate([direction[1:], none], 0)
        normal = normal + weight * (2.0 * direction - before - after)
        step_len = norm_now / total_of(direction * normal)
        filters = filters + step_len * direction
        gradient = gradient - step_len * normal
    rows = lax.broadcasted_iota(jnp.int32, (LANES, LANES), 0)
    columns = lanes_of((LANES, LANES))
    flip = (rows + columns == jnp.where(columns < TAPS, TAPS - 1, 3 * TAPS - 1)).astype(F32)
    return exact(filters, flip)


def shaped_back(taps_row, rec, spec, table, s):
    blocks = taps_row.shape[0]
    shape = threefold(jnp.concatenate([taps_row, turn(taps_row, TAPS)], 0), table("shape"))
    shape = jnp.concatenate([shape[:blocks], shape[blocks:]], 1)
    for b in range(rec.shape[2] // FB):
        rows = slice(b * FB, (b + 1) * FB)
        w_ac, w_as, w_bc, w_bs = [spec[s, i, rows, :] for i in range(4)]
        h_ac, h_as, h_bc, h_bs = [shape[b : b + 1, i * LANES : (i + 1) * LANES] for i in range(4)]
        y_ac = h_ac * w_ac - h_as * w_as - h_bc * w_bc + h_bs * w_bs
        y_as = h_ac * w_as + h_as * w_ac - h_bc * w_bs - h_bs * w_bc
        y_bc = h_ac * w_bc - h_as * w_bs + h_bc * w_ac - h_bs * w_as
        y_bs = h_ac * w_bs + h_as * w_bc + h_bc * w_as + h_bs * w_ac
        both = jnp.concatenate(
            [jnp.concatenate([y_ac, y_as], 1), jnp.concatenate([y_bc, y_bs], 1)], 0
        )
        applied = fourfold(both, table("back"))
        rec[s, 0, rows, :] = rec[s, 0, rows, :] - applied[:FB]
        rec[s, 1, rows, :] = rec[s, 1, rows, :] - applied[FB:]


def fit_kernel(
    weight,
    trace_count,
    freq_count,
    runs,
    m_any,
    rec_any,
    table_any,
    out_any,
    filters_out,
    m,
    rec,
    edge,
    halo,
    spec,
    sums,
    corner,
    corner_in,
    corner_all,
    stats,
    stats_in,
    stats_all,
    taps,
    solved,
    matrix,
    tables,
    ends_v,
    table_sem,
    m_sem,
    rec_sem,
    out_sem,
    edge_send,
    halo_sem,
    corner_send,
    corner_sem,
    relay_send,
    relay_sem,
    stats_send,
    stats_sem,
    gather_send,
    gather_sem,
    taps_send,
    taps_sem,
):
    shots = m.shape[0]
    blocks = m.shape[2] // FB
    last = trace_count - 1
    me = lax.axis_index("trace")
    layer = lax.axis_index("freq")
    owns = me < shots
    ends = ((0, 0), (1, last))

    def remote(source, target, send, arrive, **where):
        return pltpu.make_async_remote_copy(
            src_ref=source,
            dst_ref=target,
            send_sem=send,
            recv_sem=arrive,
            device_id=where,
            device_id_type=MESH,
        )

    def local(source, target, sem, s):
        return pltpu.make_async_copy(source.at[s], target.at[s], sem.at[s])

    for s in range(shots):
        local(m_any, m, m_sem, s).start()
    table_copy = pltpu.make_async_copy(table_any, tables, table_sem)
    table_copy.start()
    for s in range(shots):
        local(rec_any, rec, rec_sem, s).start()

    def table(name):
        return tables[runs[name], :]

    barrier = pltpu.get_barrier_semaphore()
    for o in range(1, trace_count):
        pl.semaphore_signal(
            barrier, inc=1, device_id={"trace": lax.rem(me + o, trace_count)}, device_id_type=MESH
        )
    for o in range(1, freq_count):
        pl.semaphore_signal(
            barrier, inc=1, device_id={"freq": lax.rem(layer + o, freq_count)}, device_id_type=MESH
        )

    @pl.when(me == 0)
    def _():
        halo[0] = jnp.zeros(halo.shape[1:], F32)

    @pl.when(me == last)
    def _():
        halo[1] = jnp.zeros(halo.shape[1:], F32)

    pl.semaphore_wait(barrier, trace_count + freq_count - 2)

    def halo_copy(side, s):
        other = jnp.minimum(me + 1, last) if side == 0 else jnp.maximum(me - 1, 0)
        return remote(
            edge.at[side, s], halo.at[side, s], edge_send.at[side, s], halo_sem.at[side, s], trace=other
        )

    def corner_copy(end, s, owner):
        return remote(corner.at[s], corner_in.at[end], corner_send.at[s], corner_sem.at[end], trace=owner)

    def relay_copy(o):
        return remote(
            corner_all.at[layer],
            corner_all.at[layer],
            relay_send.at[o],
            relay_sem.at[layer],
            freq=lax.rem(layer + o, freq_count),
        )

    def stats_copy(s):
        return remote(stats.at[s], stats_in.at[me], stats_send.at[s], stats_sem.at[me], trace=s)

    def gather_copy(o):
        return remote(
            stats_all.at[layer],
            stats_all.at[layer],
            gather_send.at[o],
            gather_sem.at[layer],
            freq=lax.rem(layer + o, freq_count),
        )

    def taps_copy(o):
        return remote(
            taps.at[me], taps.at[me], taps_send.at[o], taps_sem.at[me], trace=lax.rem(me + o, trace_count)
        )

    sends = (me < last, me > 0)
    receives = (me > 0, me < last)

    def start_halo(s):
        for side in range(2):

            @pl.when(sends[side])
            def _():
                halo_copy(side, s).start()

    def send_edges(s, carry):
        local(m_any, m, m_sem, s).wait()

        @pl.when((me == 0) | (me == last))
        def _():
            corners(m, ends_v, corner, s, me == last)
            for end, where in ends:

                @pl.when((me == where) & (s != where))
                def _():
                    corner_copy(end, s, s).start()

                @pl.when((me == where) & (s == where))
                def _():
                    corner_in[end] = corner[s]

        pack_edges(m, edge, s)
        start_halo(s)
        return carry

    lax.fori_loop(0, shots, send_edges, 0)

    def measure(s):
        local(rec_any, rec, rec_sem, s).wait()
        for side in range(2):

            @pl.when(receives[side])
            def _():
                halo_copy(side, s).wait_recv()

        statistics(m, rec, halo, spec, sums, table, s)
        stats[s, 0] = fourfold(sums[0], table("power"))
        stats[s, 1] = fourfold(sums[1], table("cross"))
        stats[s, 2] = fourfold(jnp.concatenate([sums[i] for i in range(2, 6)], 1), table("sides"))

        @pl.when(me != s)
        def _():
            stats_copy(s).start()

    def relay():
        for end, where in ends:

            @pl.when(me != where)
            def _():
                corner_copy(end, 0, me).wait_recv()

        corner_all[layer] = joined_corners(corner_in[0], corner_in[1])
        for o in range(1, freq_count):
            relay_copy(o).start()

    def prepare():
        for o in range(1, freq_count):
            other = lax.rem(layer + o, freq_count)
            remote(
                corner_all.at[other], corner_all.at[other], relay_send.at[o], relay_sem.at[other], freq=other
            ).wait_recv()
        prepare_corners(corner_all, matrix)

    def gather():
        whole = stats[me]
        for o in range(1, trace_count):
            other = lax.rem(me + o, trace_count)
            remote(
                stats.at[0], stats_in.at[other], stats_send.at[0], stats_sem.at[other], trace=other
            ).wait_recv()
            whole = whole + stats_in[other]
        stats_all[layer] = whole
        for o in range(1, freq_count):
            gather_copy(o).start()

    def solve_own():
        for o in range(1, freq_count):
            other = lax.rem(layer + o, freq_count)
            remote(
                stats_all.at[other], stats_all.at[other], gather_send.at[o], gather_sem.at[other], freq=other
            ).wait_recv()
        rows = [stats_all[:, i].reshape(freq_count * blocks, LANES) for i in range(3)]
        solved[...] = solve(weight, *rows, matrix).reshape(freq_count, blocks, LANES)
        taps[me] = solved[layer]
        for o in range(1, trace_count):
            taps_copy(o).start()

    def finish(s):
        @pl.when(me != s)
        def _():
            remote(taps.at[s], taps.at[s], taps_send.at[0], taps_sem.at[s], trace=s).wait_recv()

        own = taps[s]
        filters_out[s, 0] = own[:, :TAPS]
        filters_out[s, 1] = turn(own, TAPS)[:, :TAPS]
        shaped_back(own, rec, spec, table, s)
        local(rec, out_any, out_sem, s).start()

    relay_at = jnp.minimum(me, 1)

    def measure_step(s, carry):
        measure(s)
        pl.when(owns & (s == relay_at))(relay)
        return carry

    def finish_step(s, carry):
        finish(s)
        return carry

    table_copy.wait()
    lax.fori_loop(0, shots, measure_step, 0)

    @pl.when(owns)
    def _():
        gather()
        prepare()
        solve_own()

    lax.fori_loop(0, shots, finish_step, 0)

    def drain(s, carry):
        for side in range(2):

            @pl.when(sends[side])
            def _():
                halo_copy(side, s).wait_send()

        for end, where in ends:

            @pl.when((me == where) & (s != where))
            def _():
                corner_copy(end, s, s).wait_send()

        @pl.when(me != s)
        def _():
            stats_copy(s).wait_send()

        local(rec, out_any, out_sem, s).wait()
        return carry

    lax.fori_loop(0, shots, drain, 0)

    @pl.when(owns)
    def _():
        for o in range(1, freq_count):
            relay_copy(o).wait_send()
            gather_copy(o).wait_send()
        for o in range(1, trace_count):
            taps_copy(o).wait_send()


def body(recorded, multiples):
    shots, parts, freq_rows, trace_rows = multiples.shape
    blocks = freq_rows // FB
    trace_count, freq_count = lax.axis_size("trace"), lax.axis_size("freq")
    assert shots <= trace_count
    weight = 0.5 * FB * trace_rows * trace_count
    pack_rows = freq_rows * HALF // LANES

    table, runs = all_tables()
    field = (shots, parts, freq_rows, trace_rows)
    dma = pltpu.SemaphoreType.DMA
    vmem = pl.BlockSpec(memory_space=pltpu.VMEM)
    anywhere = pl.BlockSpec(memory_space=pl.ANY)
    return pl.pallas_call(
        functools.partial(fit_kernel, weight, trace_count, freq_count, runs),
        in_specs=[anywhere, anywhere, anywhere],
        out_specs=[anywhere, vmem],
        out_shape=[
            jax.ShapeDtypeStruct(field, F32),
            jax.ShapeDtypeStruct((shots, parts, blocks, TAPS), F32),
        ],
        scratch_shapes=[
            pltpu.VMEM(field, F32),
            pltpu.VMEM(field, F32),
            pltpu.VMEM((2, shots, parts, pack_rows, LANES), F32),
            pltpu.VMEM((2, shots, parts, pack_rows, LANES), F32),
            pltpu.VMEM((shots, 4, freq_rows, LANES), F32),
            pltpu.VMEM((6, blocks, LANES), F32),
            pltpu.VMEM((shots, HALF // 2, blocks, LANES), F32),
            pltpu.VMEM((2, HALF // 2, blocks, LANES), F32),
            pltpu.VMEM((freq_count, HALF, blocks, LANES), F32),
            pltpu.VMEM((shots, 3, blocks, LANES), F32),
            pltpu.VMEM((trace_count, 3, blocks, LANES), F32),
            pltpu.VMEM((freq_count, 3, blocks, LANES), F32),
            pltpu.VMEM((shots, blocks, LANES), F32),
            pltpu.VMEM((freq_count, blocks, LANES), F32),
            pltpu.VMEM((TAPS + 2, freq_count * blocks, LANES), F32),
            pltpu.VMEM(table.shape, BF16),
            pltpu.VMEM((freq_rows, LANES), BF16),
            dma,
            dma((shots,)),
            dma((shots,)),
            dma((shots,)),
            dma((2, shots)),
            dma((2, shots)),
            dma((shots,)),
            dma((2,)),
            dma((freq_count,)),
            dma((freq_count,)),
            dma((shots,)),
            dma((trace_count,)),
            dma((freq_count,)),
            dma((freq_count,)),
            dma((trace_count,)),
            dma((shots,)),
        ],
        compiler_params=pltpu.CompilerParams(
            collective_id=0, has_side_effects=True, vmem_limit_bytes=48000000
        ),
        name="fit",
    )(multiples, recorded, jnp.asarray(table))


def solution(mesh):
    spec = P(None, None, "freq", "trace")
    return jax.shard_map(
        body,
        mesh=mesh,
        in_specs=(spec, spec),
        out_specs=(spec, P(None, None, "freq", None)),
        check_vma=False,
    )
```

```python
import functools

import jax
import jax.numpy as jnp
import numpy as np
from jax import lax
from jax.experimental import pallas as pl
from jax.experimental.pallas import tpu as pltpu
from jax.sharding import PartitionSpec as P

FB = 64
TAPS = 64
ITERS = 3
HALF = TAPS // 2
LANES = 128
POINTS = 2 * LANES
F32 = jnp.float32
BF16 = jnp.bfloat16
MESH = pl.DeviceIdType.MESH


def lanes_of(shape):
    return lax.broadcasted_iota(jnp.int32, shape, len(shape) - 1)


def turn(value, shift):
    shift = shift % LANES
    return value if shift == 0 else pltpu.roll(value, shift, 1)


def split(value):
    high = value.astype(BF16)
    return high, (value - high.astype(F32)).astype(BF16)


def waves(positions):
    phase = (2 * np.pi / POINTS) * np.outer(np.asarray(positions), np.arange(LANES) + 0.5)
    return np.cos(phase), np.sin(phase)


def both_waves(positions):
    return np.concatenate(waves(positions), 1)


def halves(table):
    high = table.astype(np.float32).astype(BF16)
    return high, (table - high.astype(np.float64)).astype(np.float32).astype(BF16)


def all_tables():
    high, low = halves(both_waves(np.arange(LANES)))
    tail_high, tail_low = halves(both_waves(LANES + np.arange(TAPS)))
    lag = np.where(np.arange(LANES) < TAPS, np.arange(LANES), LANES - np.arange(LANES))
    used = (np.arange(LANES) != TAPS) / LANES
    sign = np.where(np.arange(LANES) < TAPS, -2.0, 2.0)
    lag_cos, lag_sin = waves(lag)
    right = both_waves(-1 - np.arange(TAPS)).T / LANES
    none = np.zeros_like(right)
    shape_high, shape_low = halves(both_waves(np.arange(TAPS)))
    parts = dict(
        wide=[high, high],
        low=[low],
        tail=[tail_high, tail_high, tail_low, np.zeros_like(tail_low)],
        power=[np.concatenate(halves(lag_cos.T * used), 1)],
        cross=[np.concatenate(halves(lag_sin.T * (sign * used)), 1)],
        sides=[np.concatenate(halves(np.block([[right, none], [none, right]])), 1)],
        shape=[shape_high, shape_high, shape_low, np.zeros_like(shape_low)],
        back=[np.concatenate(halves(both_waves(TAPS + np.arange(LANES)).T / LANES), 1)],
    )
    parts = {name: np.concatenate(part, 0) for name, part in parts.items()}
    runs, start = {}, 0
    for name, part in parts.items():
        runs[name] = slice(start, start + part.shape[0])
        start += part.shape[0]
    return np.concatenate(list(parts.values()), 0), runs


def over_first(left, right):
    return lax.dot_general(left, right, (((0,), (0,)), ((), ())), preferred_element_type=F32)


def product(left, right):
    return jnp.dot(left, right, preferred_element_type=F32)


def exact(left, right):
    return jnp.dot(left, right, precision=lax.Precision.HIGHEST, preferred_element_type=F32)


def mirror(total):
    rows = lax.broadcasted_iota(jnp.int32, (LANES, LANES), 0)
    return (rows + lanes_of((LANES, LANES)) == total).astype(F32)


def total_of(value):
    return jnp.sum(jnp.sum(value, axis=1, keepdims=True), axis=0, keepdims=True)


def column_sum(value):
    return jnp.sum(value, axis=0, keepdims=True)


def pack_edges(m, edge, s):
    freq_rows = m.shape[2]
    groups = LANES // HALF
    rows = freq_rows // groups
    lane = lanes_of((rows, LANES))
    for part in range(2):
        for side in range(2):
            packed = None
            for g in range(groups):
                shift = HALF * g + HALF if side == 0 else HALF * g
                value = turn(m[s, part, g * rows : (g + 1) * rows, :], shift)
                packed = value if packed is None else jnp.where(lane >= HALF * g, value, packed)
            edge[side, s, part] = packed


def corners(m, ends, corner, s, at_last):
    freq_rows = m.shape[2]
    wide = (freq_rows, LANES)
    lane = lanes_of(wide)
    real = pltpu.roll(m[s, 0], jnp.where(at_last, HALF, 0), 1)
    imag = pltpu.roll(m[s, 1], jnp.where(at_last, 2 * HALF, HALF), 1)
    both = jnp.where(lane < HALF, real, imag)
    rest = both - both.astype(BF16).astype(F32)
    ends[...] = jnp.where(lane < TAPS, both, turn(rest, TAPS)).astype(BF16)
    lane = lanes_of((HALF, LANES))
    for b in range(freq_rows // FB):
        part = ends[b * FB : (b + 1) * FB, :]
        gram = over_first(part, part)
        gram = gram[:TAPS] + gram[TAPS:]
        gram = gram + turn(gram, TAPS)
        one, two = gram[:HALF], turn(gram[HALF:], HALF)
        value = jnp.where(lane % TAPS < HALF, one + two, one - two)
        corner[s, :, b, :] = jnp.where(
            lane[: HALF // 2] < TAPS, value[: HALF // 2], value[HALF // 2 :]
        )


def joined_corners(left, right):
    shape = left.shape
    lane = lanes_of(shape)

    def moved(value, shift):
        return pltpu.roll(value, shift % LANES, 2)

    def pick(*values):
        result = values[0]
        for i in range(1, 4):
            result = jnp.where(lane >= i * HALF, values[i], result)
        return result

    first = pick(right, moved(left, HALF), moved(right, HALF), moved(left, TAPS))
    second = pick(moved(right, TAPS), moved(left, -HALF), moved(right, -HALF), left)
    value = jnp.concatenate([first, second], 0)
    place = lanes_of(value.shape) % TAPS
    step = 1
    while step < HALF:
        none = jnp.zeros((step,) + shape[1:], F32)
        later = jnp.concatenate([moved(value[step:], -step), none], 0)
        sooner = jnp.concatenate([none, moved(value[:-step], step)], 0)
        value = value + jnp.where(
            place < HALF - step, later, jnp.where(place >= HALF + step, sooner, 0.0)
        )
        step *= 2
    return value


def fourfold(value, table):
    count = value.shape[0]
    both = product(jnp.concatenate(split(value), 0), table)
    both = both[:count] + both[count:]
    return both[:, :LANES] + both[:, LANES:]


def threefold(value, table):
    top = value.astype(BF16)
    rest = turn(value - top.astype(F32), TAPS)
    mixed = jnp.where(lanes_of(value.shape) < TAPS, value, rest).astype(BF16)
    return product(jnp.concatenate([mixed, top], 1), table)


def statistics(m, rec, halo, spec, sums, table, s):
    freq_rows = m.shape[2]
    group_rows = freq_rows * HALF // LANES
    lane = lanes_of((FB, LANES))
    for b in range(freq_rows // FB):
        rows = slice(b * FB, (b + 1) * FB)
        group, first = (b * FB) // group_rows, (b * FB) % group_rows
        near = slice(first, first + FB)
        starts, tails = [], []
        for part in range(2):
            turned = turn(m[s, part, rows, :], HALF)
            left = turn(halo[0, s, part, near, :], -HALF * group)
            right = turn(halo[1, s, part, near, :], HALF - HALF * group)
            starts.append(jnp.where(lane < HALF, left, turned))
            tails.append(jnp.where(lane < HALF, turned, right))
        high, rest = split(jnp.concatenate(starts + [rec[s, 0, rows, :], rec[s, 1, rows, :]], 0))
        main = product(jnp.concatenate([high, rest], 1), table("wide")) + product(high, table("low"))
        last = threefold(jnp.concatenate(tails, 0), table("tail"))

        def parts(value, first):
            return value[first : first + FB, :LANES], value[first : first + FB, LANES:]

        s_all = parts(main, 0) + parts(main, FB)
        t_all = parts(last, 0) + parts(last, FB)
        r_ac, r_as, r_bc, r_bs = parts(main, 2 * FB) + parts(main, 3 * FB)
        w_all = [x + y for x, y in zip(s_all, t_all)]
        for i in range(4):
            spec[s, i, rows, :] = w_all[i]
        w_ac, w_as, w_bc, w_bs = w_all
        t_ac, t_as, t_bc, t_bs = t_all
        power = sum(x * (w + t) for x, w, t in zip(s_all, w_all, t_all))
        cross = (w_ac * w_bs - w_as * w_bc) - (t_ac * t_bs - t_as * t_bc)
        found = [
            power,
            cross,
            w_ac * r_ac + w_as * r_as + w_bc * r_bc + w_bs * r_bs,
            w_ac * r_as - w_as * r_ac + w_bc * r_bs - w_bs * r_bc,
            w_ac * r_bc + w_as * r_bs - w_bc * r_ac - w_bs * r_as,
            w_ac * r_bs - w_as * r_bc - w_bc * r_as + w_bs * r_ac,
        ]
        for i in range(6):
            sums[i, b : b + 1, :] = column_sum(found[i])


def prepare_corners(corner, matrix):
    blocks = corner.shape[0] * corner.shape[2]

    def row(r):
        return corner[:, r, :, :].reshape(blocks, LANES)

    lane = lanes_of((blocks, LANES))
    place = lane % TAPS
    is_real = lane < TAPS
    for i in range(HALF):
        value = row(i)
        if i:
            moved = jnp.where(place < HALF - 1, turn(value, -1), 0.0)
            matrix[i - 1] = jnp.where(is_real, -moved, moved)
        value = jnp.where(place < HALF, 0.0, value)
        matrix[HALF + i] = jnp.where(is_real, -value, value)
    matrix[HALF - 1] = jnp.zeros((blocks, LANES), F32)
    right = jnp.where(place < HALF, row(0), 0.0)
    add_real = jnp.where(lane < HALF, right, 0.0)
    add_imag = jnp.where(lane < HALF, turn(right, TAPS), 0.0)
    back = mirror(LANES)
    matrix[TAPS] = jnp.where(is_real, add_real, exact(add_real, back))
    matrix[TAPS + 1] = jnp.where(is_real, -add_imag, exact(add_imag, back))


def solve(weight, toep_real, toep_imag, gradient, matrix):
    blocks = gradient.shape[0]
    lane = lanes_of((blocks, LANES))
    is_real = lane < TAPS
    toep_real = toep_real + matrix[TAPS]
    toep_imag = toep_imag + matrix[TAPS + 1]
    for t in range(TAPS):
        matrix[t] += jnp.where(is_real, turn(toep_real, t), turn(toep_imag, TAPS + t))

    filters = jnp.zeros((blocks, LANES), F32)
    direction = norm_now = None
    none = jnp.zeros((1, LANES), F32)
    for iteration in range(ITERS):
        norm_next = total_of(gradient * gradient)
        if iteration == 0:
            direction = gradient
        else:
            direction = gradient + (norm_next / norm_now) * direction
        norm_now = norm_next
        by_real = jnp.zeros((blocks, LANES), F32)
        by_imag = jnp.zeros((blocks, LANES), F32)
        for t in range(TAPS):
            by_real = by_real + direction[:, t : t + 1] * matrix[t]
            by_imag = by_imag + direction[:, TAPS + t : TAPS + t + 1] * matrix[t]
        by_imag = turn(by_imag, TAPS)
        normal = by_real + jnp.where(is_real, -by_imag, by_imag)
        before = jnp.concatenate([none, direction[:-1]], 0)
        after = jnp.concatenate([direction[1:], none], 0)
        normal = normal + weight * (2.0 * direction - before - after)
        step_len = norm_now / total_of(direction * normal)
        filters = filters + step_len * direction
        gradient = gradient - step_len * normal
    rows = lax.broadcasted_iota(jnp.int32, (LANES, LANES), 0)
    columns = lanes_of((LANES, LANES))
    flip = (rows + columns == jnp.where(columns < TAPS, TAPS - 1, 3 * TAPS - 1)).astype(F32)
    return exact(filters, flip)


def shapes(taps, table):
    shots, blocks, _ = taps.shape
    rows = taps.reshape(shots * blocks, LANES)
    value = threefold(jnp.concatenate([rows, turn(rows, TAPS)], 0), table("shape"))
    value = jnp.concatenate([value[: shots * blocks], value[shots * blocks :]], 1)
    return value.reshape(shots, blocks, 2 * POINTS)


def shaped_back(shape, rec, spec, table, s):
    for b in range(rec.shape[2] // FB):
        rows = slice(b * FB, (b + 1) * FB)
        w_ac, w_as, w_bc, w_bs = [spec[s, i, rows, :] for i in range(4)]
        h_ac, h_as, h_bc, h_bs = [shape[b : b + 1, i * LANES : (i + 1) * LANES] for i in range(4)]
        y_ac = h_ac * w_ac - h_as * w_as - h_bc * w_bc + h_bs * w_bs
        y_as = h_ac * w_as + h_as * w_ac - h_bc * w_bs - h_bs * w_bc
        y_bc = h_ac * w_bc - h_as * w_bs + h_bc * w_ac - h_bs * w_as
        y_bs = h_ac * w_bs + h_as * w_bc + h_bc * w_as + h_bs * w_ac
        both = jnp.concatenate(
            [jnp.concatenate([y_ac, y_as], 1), jnp.concatenate([y_bc, y_bs], 1)], 0
        )
        applied = fourfold(both, table("back"))
        rec[s, 0, rows, :] = rec[s, 0, rows, :] - applied[:FB]
        rec[s, 1, rows, :] = rec[s, 1, rows, :] - applied[FB:]


def detour_count(shots, trace_count):
    return (shots - 1) // 2 if trace_count >= 4 else 0


def fit_kernel(
    weight,
    trace_count,
    freq_count,
    runs,
    m_any,
    rec_any,
    table_any,
    out_any,
    filters_out,
    m,
    rec,
    edge,
    halo,
    spec,
    sums,
    corner,
    corner_in,
    corner_all,
    stats,
    stats_in,
    stats_all,
    taps,
    solved,
    matrix,
    tables,
    ends_v,
    passing,
    pass_send,
    pass_sem,
    table_sem,
    m_sem,
    rec_sem,
    out_sem,
    edge_send,
    halo_sem,
    corner_send,
    corner_sem,
    relay_send,
    relay_sem,
    stats_send,
    stats_sem,
    gather_send,
    gather_sem,
    taps_send,
    taps_sem,
):
    shots = m.shape[0]
    blocks = m.shape[2] // FB
    last = trace_count - 1
    me = lax.axis_index("trace")
    layer = lax.axis_index("freq")
    owns = me < shots
    ends = ((0, 0), (1, last))

    def remote(source, target, send, arrive, **where):
        return pltpu.make_async_remote_copy(
            src_ref=source,
            dst_ref=target,
            send_sem=send,
            recv_sem=arrive,
            device_id=where,
            device_id_type=MESH,
        )

    def local(source, target, sem, s):
        return pltpu.make_async_copy(source.at[s], target.at[s], sem.at[s])

    for s in range(shots):
        local(m_any, m, m_sem, s).start()
    table_copy = pltpu.make_async_copy(table_any, tables, table_sem)
    table_copy.start()
    for s in range(shots):
        local(rec_any, rec, rec_sem, s).start()

    def table(name):
        return tables[runs[name], :]

    barrier = pltpu.get_barrier_semaphore()
    for o in range(1, trace_count):
        pl.semaphore_signal(
            barrier, inc=1, device_id={"trace": lax.rem(me + o, trace_count)}, device_id_type=MESH
        )
    for o in range(1, freq_count):
        pl.semaphore_signal(
            barrier, inc=1, device_id={"freq": lax.rem(layer + o, freq_count)}, device_id_type=MESH
        )

    @pl.when(me == 0)
    def _():
        halo[0] = jnp.zeros(halo.shape[1:], F32)

    @pl.when(me == last)
    def _():
        halo[1] = jnp.zeros(halo.shape[1:], F32)

    pl.semaphore_wait(barrier, trace_count + freq_count - 2)

    def halo_copy(side, s):
        other = jnp.minimum(me + 1, last) if side == 0 else jnp.maximum(me - 1, 0)
        return remote(
            edge.at[side, s], halo.at[side, s], edge_send.at[side, s], halo_sem.at[side, s], trace=other
        )

    def corner_copy(end, s, owner):
        return remote(corner.at[s], corner_in.at[end], corner_send.at[s], corner_sem.at[end], trace=owner)

    def relay_copy(o):
        return remote(
            corner_all.at[layer],
            corner_all.at[layer],
            relay_send.at[o],
            relay_sem.at[layer],
            freq=lax.rem(layer + o, freq_count),
        )

    def stats_copy(s):
        return remote(stats.at[s], stats_in.at[me], stats_send.at[s], stats_sem.at[me], trace=s)

    def gather_copy(o):
        return remote(
            stats_all.at[layer],
            stats_all.at[layer],
            gather_send.at[o],
            gather_sem.at[layer],
            freq=lax.rem(layer + o, freq_count),
        )

    def taps_copy(o):
        return remote(
            taps.at[me], taps.at[me], taps_send.at[o], taps_sem.at[me], trace=lax.rem(me + o, trace_count)
        )

    sends = (me < last, me > 0)
    receives = (me > 0, me < last)

    middle = trace_count // 2
    detours = detour_count(shots, trace_count)

    def detoured(side, s):
        if not detours:
            return False
        return (me == (middle - 1 if side == 0 else middle)) & (s > 0) & (lax.rem(s, 2) == 0)

    def detour_copy(side, s):
        i = jnp.maximum(s // 2 - 1, 0)
        return remote(
            edge.at[side, s],
            passing.at[i],
            edge_send.at[side, s],
            pass_sem.at[i],
            trace=last if side == 0 else 0,
        )

    def pass_copy(side, i):
        s = 2 * i + 2
        return remote(
            passing.at[i],
            halo.at[side, s],
            pass_send.at[i],
            halo_sem.at[side, s],
            trace=middle if side == 0 else middle - 1,
        )

    passes = (me == last, me == 0)

    def start_halo(s):
        for side in range(2):

            @pl.when(sends[side] & jnp.logical_not(detoured(side, s)))
            def _():
                halo_copy(side, s).start()

            @pl.when(detoured(side, s))
            def _():
                detour_copy(side, s).start()

    def pass_on(i):
        for side in range(2):

            @pl.when(passes[side])
            def _():
                detour_copy(side, 2 * i + 2).wait_recv()
                pass_copy(side, i).start()

    @pl.when((me == 0) | (me == last))
    def _():
        def send_corners(s, carry):
            local(m_any, m, m_sem, s).wait()
            corners(m, ends_v, corner, s, me == last)
            for end, where in ends:

                @pl.when((me == where) & (s != where))
                def _():
                    corner_copy(end, s, s).start()

                @pl.when((me == where) & (s == where))
                def _():
                    corner_in[end] = corner[s]

            return carry

        lax.fori_loop(0, shots, send_corners, 0)

    def send_edges(s, carry):
        @pl.when((me > 0) & (me < last))
        def _():
            local(m_any, m, m_sem, s).wait()

        pack_edges(m, edge, s)
        start_halo(s)
        return carry

    lax.fori_loop(0, shots, send_edges, 0)
    for i in range(detours):
        pass_on(i)

    def measure(s):
        local(rec_any, rec, rec_sem, s).wait()
        for side in range(2):

            @pl.when(receives[side])
            def _():
                halo_copy(side, s).wait_recv()

        statistics(m, rec, halo, spec, sums, table, s)
        stats[s, 0] = fourfold(sums[0], table("power"))
        stats[s, 1] = fourfold(sums[1], table("cross"))
        stats[s, 2] = fourfold(jnp.concatenate([sums[i] for i in range(2, 6)], 1), table("sides"))

        @pl.when(me != s)
        def _():
            stats_copy(s).start()

    def relay():
        for end, where in ends:

            @pl.when(me != where)
            def _():
                corner_copy(end, 0, me).wait_recv()

        corner_all[layer] = joined_corners(corner_in[0], corner_in[1])
        for o in range(1, freq_count):
            relay_copy(o).start()

    def prepare():
        for o in range(1, freq_count):
            other = lax.rem(layer + o, freq_count)
            remote(
                corner_all.at[other], corner_all.at[other], relay_send.at[o], relay_sem.at[other], freq=other
            ).wait_recv()
        prepare_corners(corner_all, matrix)

    def gather():
        whole = stats[me]
        for o in range(1, trace_count):
            other = lax.rem(me + o, trace_count)
            remote(
                stats.at[0], stats_in.at[other], stats_send.at[0], stats_sem.at[other], trace=other
            ).wait_recv()
            whole = whole + stats_in[other]
        stats_all[layer] = whole
        for o in range(1, freq_count):
            gather_copy(o).start()

    def solve_own():
        for o in range(1, freq_count):
            other = lax.rem(layer + o, freq_count)
            remote(
                stats_all.at[other], stats_all.at[other], gather_send.at[o], gather_sem.at[other], freq=other
            ).wait_recv()
        rows = [stats_all[:, i].reshape(freq_count * blocks, LANES) for i in range(3)]
        solved[...] = solve(weight, *rows, matrix).reshape(freq_count, blocks, LANES)
        taps[me] = solved[layer]
        for o in range(1, trace_count):
            taps_copy(o).start()

    def take_taps(s):
        @pl.when(me != s)
        def _():
            remote(taps.at[s], taps.at[s], taps_send.at[0], taps_sem.at[s], trace=s).wait_recv()

        own = taps[s]
        filters_out[s, 0] = own[:, :TAPS]
        filters_out[s, 1] = turn(own, TAPS)[:, :TAPS]

    at_once = 2 if shots % 2 == 0 else 1

    def finish(i, carry):
        group = [i * at_once + s for s in range(at_once)]
        for s in group:
            take_taps(s)
        shaped = shapes(taps[pl.ds(i * at_once, at_once)], table)
        for s in range(at_once):
            shaped_back(shaped[s], rec, spec, table, group[s])
        for s in group:
            local(rec, out_any, out_sem, s).start()
        return carry

    relay_at = jnp.minimum(me, 2)

    def measure_step(s, carry):
        measure(s)
        pl.when(owns & (s == relay_at))(relay)
        return carry

    table_copy.wait()
    lax.fori_loop(0, shots, measure_step, 0)

    @pl.when(owns)
    def _():
        gather()
        prepare()
        solve_own()

    lax.fori_loop(0, shots // at_once, finish, 0)

    def drain(s, carry):
        for side in range(2):

            @pl.when(sends[side] & jnp.logical_not(detoured(side, s)))
            def _():
                halo_copy(side, s).wait_send()

            @pl.when(detoured(side, s))
            def _():
                detour_copy(side, s).wait_send()

            @pl.when(passes[side] & (s < detours))
            def _():
                pass_copy(side, jnp.minimum(s, detours - 1)).wait_send()

        for end, where in ends:

            @pl.when((me == where) & (s != where))
            def _():
                corner_copy(end, s, s).wait_send()

        @pl.when(me != s)
        def _():
            stats_copy(s).wait_send()

        local(rec, out_any, out_sem, s).wait()
        return carry

    lax.fori_loop(0, shots, drain, 0)

    @pl.when(owns)
    def _():
        for o in range(1, freq_count):
            relay_copy(o).wait_send()
            gather_copy(o).wait_send()
        for o in range(1, trace_count):
            taps_copy(o).wait_send()


def body(recorded, multiples):
    shots, parts, freq_rows, trace_rows = multiples.shape
    blocks = freq_rows // FB
    trace_count, freq_count = lax.axis_size("trace"), lax.axis_size("freq")
    assert shots <= trace_count
    weight = 0.5 * FB * trace_rows * trace_count
    pack_rows = freq_rows * HALF // LANES
    detours = detour_count(shots, trace_count)

    table, runs = all_tables()
    field = (shots, parts, freq_rows, trace_rows)
    dma = pltpu.SemaphoreType.DMA
    vmem = pl.BlockSpec(memory_space=pltpu.VMEM)
    anywhere = pl.BlockSpec(memory_space=pl.ANY)
    return pl.pallas_call(
        functools.partial(fit_kernel, weight, trace_count, freq_count, runs),
        in_specs=[anywhere, anywhere, anywhere],
        out_specs=[anywhere, vmem],
        out_shape=[
            jax.ShapeDtypeStruct(field, F32),
            jax.ShapeDtypeStruct((shots, parts, blocks, TAPS), F32),
        ],
        scratch_shapes=[
            pltpu.VMEM(field, F32),
            pltpu.VMEM(field, F32),
            pltpu.VMEM((2, shots, parts, pack_rows, LANES), F32),
            pltpu.VMEM((2, shots, parts, pack_rows, LANES), F32),
            pltpu.VMEM((shots, 4, freq_rows, LANES), F32),
            pltpu.VMEM((6, blocks, LANES), F32),
            pltpu.VMEM((shots, HALF // 2, blocks, LANES), F32),
            pltpu.VMEM((2, HALF // 2, blocks, LANES), F32),
            pltpu.VMEM((freq_count, HALF, blocks, LANES), F32),
            pltpu.VMEM((shots, 3, blocks, LANES), F32),
            pltpu.VMEM((trace_count, 3, blocks, LANES), F32),
            pltpu.VMEM((freq_count, 3, blocks, LANES), F32),
            pltpu.VMEM((shots, blocks, LANES), F32),
            pltpu.VMEM((freq_count, blocks, LANES), F32),
            pltpu.VMEM((TAPS + 2, freq_count * blocks, LANES), F32),
            pltpu.VMEM(table.shape, BF16),
            pltpu.VMEM((freq_rows, LANES), BF16),
            pltpu.VMEM((max(detours, 1), parts, pack_rows, LANES), F32),
            dma((max(detours, 1),)),
            dma((max(detours, 1),)),
            dma,
            dma((shots,)),
            dma((shots,)),
            dma((shots,)),
            dma((2, shots)),
            dma((2, shots)),
            dma((shots,)),
            dma((2,)),
            dma((freq_count,)),
            dma((freq_count,)),
            dma((shots,)),
            dma((trace_count,)),
            dma((freq_count,)),
            dma((freq_count,)),
            dma((trace_count,)),
            dma((shots,)),
        ],
        compiler_params=pltpu.CompilerParams(
            collective_id=0, has_side_effects=True, vmem_limit_bytes=48000000
        ),
        name="fit",
    )(multiples, recorded, jnp.asarray(table))


def solution(mesh):
    spec = P(None, None, "freq", "trace")
    return jax.shard_map(
        body,
        mesh=mesh,
        in_specs=(spec, spec),
        out_specs=(spec, P(None, None, "freq", None)),
        check_vma=False,
    )
```

```python
import functools

import jax
import jax.numpy as jnp
import numpy as np
from jax import lax
from jax.experimental import pallas as pl
from jax.experimental.pallas import tpu as pltpu
from jax.sharding import PartitionSpec as P

FB = 64
TAPS = 64
ITERS = 3
HALF = TAPS // 2
LANES = 128
POINTS = 2 * LANES
F32 = jnp.float32
BF16 = jnp.bfloat16
MESH = pl.DeviceIdType.MESH


def lanes_of(shape):
    return lax.broadcasted_iota(jnp.int32, shape, len(shape) - 1)


def turn(value, shift):
    shift = shift % LANES
    return value if shift == 0 else pltpu.roll(value, shift, 1)


def split(value):
    high = value.astype(BF16)
    return high, (value - high.astype(F32)).astype(BF16)


def waves(positions):
    phase = (2 * np.pi / POINTS) * np.outer(np.asarray(positions), np.arange(LANES) + 0.5)
    return np.cos(phase), np.sin(phase)


def both_waves(positions):
    return np.concatenate(waves(positions), 1)


def halves(table):
    high = table.astype(np.float32).astype(BF16)
    return high, (table - high.astype(np.float64)).astype(np.float32).astype(BF16)


def all_tables():
    high, low = halves(both_waves(np.arange(LANES)))
    tail_high, tail_low = halves(both_waves(LANES + np.arange(TAPS)))
    lag = np.where(np.arange(LANES) < TAPS, np.arange(LANES), LANES - np.arange(LANES))
    used = (np.arange(LANES) != TAPS) / LANES
    sign = np.where(np.arange(LANES) < TAPS, -2.0, 2.0)
    lag_cos, lag_sin = waves(lag)
    right = both_waves(-1 - np.arange(TAPS)).T / LANES
    none = np.zeros_like(right)
    shape_high, shape_low = halves(both_waves(np.arange(TAPS)))
    parts = dict(
        wide=[high, high],
        low=[low],
        tail=[tail_high, tail_high, tail_low, np.zeros_like(tail_low)],
        power=[np.concatenate(halves(lag_cos.T * used), 1)],
        cross=[np.concatenate(halves(lag_sin.T * (sign * used)), 1)],
        sides=[np.concatenate(halves(np.block([[right, none], [none, right]])), 1)],
        shape=[shape_high, shape_high, shape_low, np.zeros_like(shape_low)],
        back=[np.concatenate(halves(both_waves(TAPS + np.arange(LANES)).T / LANES), 1)],
    )
    parts = {name: np.concatenate(part, 0) for name, part in parts.items()}
    runs, start = {}, 0
    for name, part in parts.items():
        runs[name] = slice(start, start + part.shape[0])
        start += part.shape[0]
    return np.concatenate(list(parts.values()), 0), runs


def over_first(left, right):
    return lax.dot_general(left, right, (((0,), (0,)), ((), ())), preferred_element_type=F32)


def product(left, right):
    return jnp.dot(left, right, preferred_element_type=F32)


def exact(left, right):
    return jnp.dot(left, right, precision=lax.Precision.HIGHEST, preferred_element_type=F32)


def mirror(total):
    rows = lax.broadcasted_iota(jnp.int32, (LANES, LANES), 0)
    return (rows + lanes_of((LANES, LANES)) == total).astype(F32)


def total_of(value):
    return jnp.sum(jnp.sum(value, axis=0, keepdims=True), axis=1, keepdims=True)


def column_sum(value):
    return jnp.sum(value, axis=0, keepdims=True)


def pack_edges(m, edge, s):
    freq_rows = m.shape[2]
    groups = LANES // HALF
    rows = freq_rows // groups
    lane = lanes_of((rows, LANES))
    for part in range(2):
        for side in range(2):
            packed = None
            for g in range(groups):
                shift = HALF * g + HALF if side == 0 else HALF * g
                value = turn(m[s, part, g * rows : (g + 1) * rows, :], shift)
                packed = value if packed is None else jnp.where(lane >= HALF * g, value, packed)
            edge[side, s, part] = packed


def corners(m, ends, corner, s, at_last):
    freq_rows = m.shape[2]
    wide = (freq_rows, LANES)
    lane = lanes_of(wide)
    real = pltpu.roll(m[s, 0], jnp.where(at_last, HALF, 0), 1)
    imag = pltpu.roll(m[s, 1], jnp.where(at_last, 2 * HALF, HALF), 1)
    both = jnp.where(lane < HALF, real, imag)
    rest = both - both.astype(BF16).astype(F32)
    ends[...] = jnp.where(lane < TAPS, both, turn(rest, TAPS)).astype(BF16)
    lane = lanes_of((HALF, LANES))
    for b in range(freq_rows // FB):
        part = ends[b * FB : (b + 1) * FB, :]
        gram = over_first(part, part)
        gram = gram[:TAPS] + gram[TAPS:]
        gram = gram + turn(gram, TAPS)
        one, two = gram[:HALF], turn(gram[HALF:], HALF)
        value = jnp.where(lane % TAPS < HALF, one + two, one - two)
        corner[s, :, b, :] = jnp.where(
            lane[: HALF // 2] < TAPS, value[: HALF // 2], value[HALF // 2 :]
        )


def joined_corners(left, right):
    shape = left.shape
    lane = lanes_of(shape)

    def moved(value, shift):
        return pltpu.roll(value, shift % LANES, 2)

    def pick(*values):
        result = values[0]
        for i in range(1, 4):
            result = jnp.where(lane >= i * HALF, values[i], result)
        return result

    first = pick(right, moved(left, HALF), moved(right, HALF), moved(left, TAPS))
    second = pick(moved(right, TAPS), moved(left, -HALF), moved(right, -HALF), left)
    value = jnp.concatenate([first, second], 0)
    place = lanes_of(value.shape) % TAPS
    step = 1
    while step < HALF:
        none = jnp.zeros((step,) + shape[1:], F32)
        later = jnp.concatenate([moved(value[step:], -step), none], 0)
        sooner = jnp.concatenate([none, moved(value[:-step], step)], 0)
        value = value + jnp.where(
            place < HALF - step, later, jnp.where(place >= HALF + step, sooner, 0.0)
        )
        step *= 2
    return value


def fourfold(value, table):
    count = value.shape[0]
    both = product(jnp.concatenate(split(value), 0), table)
    both = both[:count] + both[count:]
    return both[:, :LANES] + both[:, LANES:]


def threefold(value, table):
    top = value.astype(BF16)
    rest = turn(value - top.astype(F32), TAPS)
    mixed = jnp.where(lanes_of(value.shape) < TAPS, value, rest).astype(BF16)
    return product(jnp.concatenate([mixed, top], 1), table)


def statistics(m, rec, halo, spec, sums, table, s):
    freq_rows = m.shape[2]
    group_rows = freq_rows * HALF // LANES
    lane = lanes_of((FB, LANES))
    for b in range(freq_rows // FB):
        rows = slice(b * FB, (b + 1) * FB)
        group, first = (b * FB) // group_rows, (b * FB) % group_rows
        near = slice(first, first + FB)
        starts, tails = [], []
        for part in range(2):
            turned = turn(m[s, part, rows, :], HALF)
            left = turn(halo[0, s, part, near, :], -HALF * group)
            right = turn(halo[1, s, part, near, :], HALF - HALF * group)
            starts.append(jnp.where(lane < HALF, left, turned))
            tails.append(jnp.where(lane < HALF, turned, right))
        high, rest = split(jnp.concatenate(starts + [rec[s, 0, rows, :], rec[s, 1, rows, :]], 0))
        main = product(jnp.concatenate([high, rest], 1), table("wide")) + product(high, table("low"))
        last = threefold(jnp.concatenate(tails, 0), table("tail"))

        def parts(value, first):
            return value[first : first + FB, :LANES], value[first : first + FB, LANES:]

        s_all = parts(main, 0) + parts(main, FB)
        t_all = parts(last, 0) + parts(last, FB)
        r_ac, r_as, r_bc, r_bs = parts(main, 2 * FB) + parts(main, 3 * FB)
        w_all = [x + y for x, y in zip(s_all, t_all)]
        for i in range(4):
            spec[s, i, rows, :] = w_all[i]
        w_ac, w_as, w_bc, w_bs = w_all
        t_ac, t_as, t_bc, t_bs = t_all
        power = sum(x * (w + t) for x, w, t in zip(s_all, w_all, t_all))
        cross = (w_ac * w_bs - w_as * w_bc) - (t_ac * t_bs - t_as * t_bc)
        found = [
            power,
            cross,
            w_ac * r_ac + w_as * r_as + w_bc * r_bc + w_bs * r_bs,
            w_ac * r_as - w_as * r_ac + w_bc * r_bs - w_bs * r_bc,
            w_ac * r_bc + w_as * r_bs - w_bc * r_ac - w_bs * r_as,
            w_ac * r_bs - w_as * r_bc - w_bc * r_as + w_bs * r_ac,
        ]
        for i in range(6):
            sums[i, b : b + 1, :] = column_sum(found[i])


def prepare_corners(corner, matrix):
    blocks = corner.shape[0] * corner.shape[2]

    def row(r):
        return corner[:, r, :, :].reshape(blocks, LANES)

    lane = lanes_of((blocks, LANES))
    place = lane % TAPS
    is_real = lane < TAPS
    for i in range(HALF):
        value = row(i)
        if i:
            moved = jnp.where(place < HALF - 1, turn(value, -1), 0.0)
            matrix[i - 1] = jnp.where(is_real, -moved, moved)
        value = jnp.where(place < HALF, 0.0, value)
        matrix[HALF + i] = jnp.where(is_real, -value, value)
    matrix[HALF - 1] = jnp.zeros((blocks, LANES), F32)
    right = jnp.where(place < HALF, row(0), 0.0)
    add_real = jnp.where(lane < HALF, right, 0.0)
    add_imag = jnp.where(lane < HALF, turn(right, TAPS), 0.0)
    back = mirror(LANES)
    matrix[TAPS] = jnp.where(is_real, add_real, exact(add_real, back))
    matrix[TAPS + 1] = jnp.where(is_real, -add_imag, exact(add_imag, back))


def turn_matrix(matrix, square):
    groups = LANES // matrix.shape[1]
    run = TAPS // groups
    for k in range(run):
        square[k] = jnp.concatenate([matrix[g * run + k] for g in range(groups)], 0).T


def solve(weight, toep_real, toep_imag, gradient, matrix, square, lags):
    blocks = gradient.shape[0]
    groups = LANES // blocks
    run = TAPS // groups
    toep_real = toep_real + matrix[TAPS]
    toep_imag = toep_imag + matrix[TAPS + 1]
    for i, toep in enumerate((toep_real, toep_imag)):
        base = jnp.concatenate([turn(toep, g * run) for g in range(groups)], 0).T
        lags[i, :run] = base[LANES - run :]
        lags[i, run:] = base[:TAPS]
    for k in range(run):
        square[k, :TAPS] += lags[0, run - k : run - k + TAPS]
        square[k, TAPS:] += lags[1, run - k : run - k + TAPS]

    shape = (LANES, LANES)
    place = lanes_of(shape) % blocks
    lane = lanes_of((run, LANES))

    def grouped(rows):
        result = rows[:run]
        for g in range(1, groups):
            result = jnp.where(lane >= g * blocks, rows[g * run : (g + 1) * run], result)
        return result

    gradient = jnp.concatenate([gradient] * groups, 0).T
    filters = jnp.zeros(shape, F32)
    direction = norm_now = None
    for iteration in range(ITERS):
        norm_next = total_of(gradient * gradient) * (1.0 / groups)
        if iteration == 0:
            direction = gradient
        else:
            direction = gradient + (norm_next / norm_now) * direction
        norm_now = norm_next
        real, imag = grouped(direction[:TAPS]), grouped(direction[TAPS:])
        by_real = jnp.zeros(shape, F32)
        by_imag = jnp.zeros(shape, F32)
        for k in range(run):
            by_real = by_real + square[k] * real[k : k + 1]
            by_imag = by_imag + square[k] * imag[k : k + 1]
        normal = jnp.concatenate([by_real[:TAPS] - by_imag[TAPS:], by_real[TAPS:] + by_imag[:TAPS]], 0)
        shift = LANES // 2
        while shift >= blocks:
            normal = normal + turn(normal, shift)
            shift //= 2
        before = jnp.where(place == 0, 0.0, turn(direction, 1))
        after = jnp.where(place == blocks - 1, 0.0, turn(direction, -1))
        normal = normal + weight * (2.0 * direction - before - after)
        step_len = norm_now / (total_of(direction * normal) * (1.0 / groups))
        filters = filters + step_len * direction
        gradient = gradient - step_len * normal
    filters = filters.T[:blocks]
    rows = lax.broadcasted_iota(jnp.int32, (LANES, LANES), 0)
    columns = lanes_of((LANES, LANES))
    flip = (rows + columns == jnp.where(columns < TAPS, TAPS - 1, 3 * TAPS - 1)).astype(F32)
    return exact(filters, flip)


def shapes(taps, table):
    shots, blocks, _ = taps.shape
    rows = taps.reshape(shots * blocks, LANES)
    value = threefold(jnp.concatenate([rows, turn(rows, TAPS)], 0), table("shape"))
    value = jnp.concatenate([value[: shots * blocks], value[shots * blocks :]], 1)
    return value.reshape(shots, blocks, 2 * POINTS)


def shaped_back(shape, rec, spec, table, s):
    for b in range(rec.shape[2] // FB):
        rows = slice(b * FB, (b + 1) * FB)
        w_ac, w_as, w_bc, w_bs = [spec[s, i, rows, :] for i in range(4)]
        h_ac, h_as, h_bc, h_bs = [shape[b : b + 1, i * LANES : (i + 1) * LANES] for i in range(4)]
        y_ac = h_ac * w_ac - h_as * w_as - h_bc * w_bc + h_bs * w_bs
        y_as = h_ac * w_as + h_as * w_ac - h_bc * w_bs - h_bs * w_bc
        y_bc = h_ac * w_bc - h_as * w_bs + h_bc * w_ac - h_bs * w_as
        y_bs = h_ac * w_bs + h_as * w_bc + h_bc * w_as + h_bs * w_ac
        both = jnp.concatenate(
            [jnp.concatenate([y_ac, y_as], 1), jnp.concatenate([y_bc, y_bs], 1)], 0
        )
        applied = fourfold(both, table("back"))
        rec[s, 0, rows, :] = rec[s, 0, rows, :] - applied[:FB]
        rec[s, 1, rows, :] = rec[s, 1, rows, :] - applied[FB:]


def detour_count(shots, trace_count):
    return (shots - 1) // 2 if trace_count >= 4 else 0


def fit_kernel(
    weight,
    trace_count,
    freq_count,
    runs,
    m_any,
    rec_any,
    table_any,
    out_any,
    filters_out,
    m,
    rec,
    edge,
    halo,
    spec,
    sums,
    corner,
    corner_in,
    corner_all,
    stats,
    stats_in,
    stats_all,
    taps,
    solved,
    matrix,
    square,
    lags,
    tables,
    ends_v,
    passing,
    pass_send,
    pass_sem,
    table_sem,
    m_sem,
    rec_sem,
    out_sem,
    edge_send,
    halo_sem,
    corner_send,
    corner_sem,
    relay_send,
    relay_sem,
    stats_send,
    stats_sem,
    gather_send,
    gather_sem,
    taps_send,
    taps_sem,
):
    shots = m.shape[0]
    blocks = m.shape[2] // FB
    last = trace_count - 1
    me = lax.axis_index("trace")
    layer = lax.axis_index("freq")
    owns = me < shots
    ends = ((0, 0), (1, last))

    def remote(source, target, send, arrive, **where):
        return pltpu.make_async_remote_copy(
            src_ref=source,
            dst_ref=target,
            send_sem=send,
            recv_sem=arrive,
            device_id=where,
            device_id_type=MESH,
        )

    def local(source, target, sem, s):
        return pltpu.make_async_copy(source.at[s], target.at[s], sem.at[s])

    for s in range(shots):
        local(m_any, m, m_sem, s).start()
    table_copy = pltpu.make_async_copy(table_any, tables, table_sem)
    table_copy.start()
    for s in range(shots):
        local(rec_any, rec, rec_sem, s).start()

    def table(name):
        return tables[runs[name], :]

    barrier = pltpu.get_barrier_semaphore()
    for o in range(1, trace_count):
        pl.semaphore_signal(
            barrier, inc=1, device_id={"trace": lax.rem(me + o, trace_count)}, device_id_type=MESH
        )
    for o in range(1, freq_count):
        pl.semaphore_signal(
            barrier, inc=1, device_id={"freq": lax.rem(layer + o, freq_count)}, device_id_type=MESH
        )

    @pl.when(me == 0)
    def _():
        halo[0] = jnp.zeros(halo.shape[1:], F32)

    @pl.when(me == last)
    def _():
        halo[1] = jnp.zeros(halo.shape[1:], F32)

    pl.semaphore_wait(barrier, trace_count + freq_count - 2)

    def halo_copy(side, s):
        other = jnp.minimum(me + 1, last) if side == 0 else jnp.maximum(me - 1, 0)
        return remote(
            edge.at[side, s], halo.at[side, s], edge_send.at[side, s], halo_sem.at[side, s], trace=other
        )

    def corner_copy(end, s, owner):
        return remote(corner.at[s], corner_in.at[end], corner_send.at[s], corner_sem.at[end], trace=owner)

    def relay_copy(o):
        return remote(
            corner_all.at[layer],
            corner_all.at[layer],
            relay_send.at[o],
            relay_sem.at[layer],
            freq=lax.rem(layer + o, freq_count),
        )

    def stats_copy(s):
        return remote(stats.at[s], stats_in.at[me], stats_send.at[s], stats_sem.at[me], trace=s)

    def gather_copy(o):
        return remote(
            stats_all.at[layer],
            stats_all.at[layer],
            gather_send.at[o],
            gather_sem.at[layer],
            freq=lax.rem(layer + o, freq_count),
        )

    def taps_copy(o):
        return remote(
            taps.at[me], taps.at[me], taps_send.at[o], taps_sem.at[me], trace=lax.rem(me + o, trace_count)
        )

    sends = (me < last, me > 0)
    receives = (me > 0, me < last)

    middle = trace_count // 2
    detours = detour_count(shots, trace_count)

    def detoured(side, s):
        if not detours:
            return False
        return (me == (middle - 1 if side == 0 else middle)) & (s > 0) & (lax.rem(s, 2) == 0)

    def detour_copy(side, s):
        i = jnp.maximum(s // 2 - 1, 0)
        return remote(
            edge.at[side, s],
            passing.at[i],
            edge_send.at[side, s],
            pass_sem.at[i],
            trace=last if side == 0 else 0,
        )

    def pass_copy(side, i):
        s = 2 * i + 2
        return remote(
            passing.at[i],
            halo.at[side, s],
            pass_send.at[i],
            halo_sem.at[side, s],
            trace=middle if side == 0 else middle - 1,
        )

    passes = (me == last, me == 0)

    def start_halo(s):
        for side in range(2):

            @pl.when(sends[side] & jnp.logical_not(detoured(side, s)))
            def _():
                halo_copy(side, s).start()

            @pl.when(detoured(side, s))
            def _():
                detour_copy(side, s).start()

    def pass_on(i):
        for side in range(2):

            @pl.when(passes[side])
            def _():
                detour_copy(side, 2 * i + 2).wait_recv()
                pass_copy(side, i).start()

    @pl.when((me == 0) | (me == last))
    def _():
        def send_corners(s, carry):
            local(m_any, m, m_sem, s).wait()
            corners(m, ends_v, corner, s, me == last)
            for end, where in ends:

                @pl.when((me == where) & (s != where))
                def _():
                    corner_copy(end, s, s).start()

                @pl.when((me == where) & (s == where))
                def _():
                    corner_in[end] = corner[s]

            return carry

        lax.fori_loop(0, shots, send_corners, 0)

    def send_edges(s, carry):
        @pl.when((me > 0) & (me < last))
        def _():
            local(m_any, m, m_sem, s).wait()

        pack_edges(m, edge, s)
        start_halo(s)
        return carry

    lax.fori_loop(0, shots, send_edges, 0)
    for i in range(detours):
        pass_on(i)

    def measure(s):
        local(rec_any, rec, rec_sem, s).wait()
        for side in range(2):

            @pl.when(receives[side])
            def _():
                halo_copy(side, s).wait_recv()

        statistics(m, rec, halo, spec, sums, table, s)
        stats[s, 0] = fourfold(sums[0], table("power"))
        stats[s, 1] = fourfold(sums[1], table("cross"))
        stats[s, 2] = fourfold(jnp.concatenate([sums[i] for i in range(2, 6)], 1), table("sides"))

        @pl.when(me != s)
        def _():
            stats_copy(s).start()

    def relay():
        for end, where in ends:

            @pl.when(me != where)
            def _():
                corner_copy(end, 0, me).wait_recv()

        corner_all[layer] = joined_corners(corner_in[0], corner_in[1])
        for o in range(1, freq_count):
            relay_copy(o).start()

    def prepare():
        for o in range(1, freq_count):
            other = lax.rem(layer + o, freq_count)
            remote(
                corner_all.at[other], corner_all.at[other], relay_send.at[o], relay_sem.at[other], freq=other
            ).wait_recv()
        prepare_corners(corner_all, matrix)
        turn_matrix(matrix, square)

    def gather():
        whole = stats[me]
        for o in range(1, trace_count):
            other = lax.rem(me + o, trace_count)
            remote(
                stats.at[0], stats_in.at[other], stats_send.at[0], stats_sem.at[other], trace=other
            ).wait_recv()
            whole = whole + stats_in[other]
        stats_all[layer] = whole
        for o in range(1, freq_count):
            gather_copy(o).start()

    def solve_own():
        for o in range(1, freq_count):
            other = lax.rem(layer + o, freq_count)
            remote(
                stats_all.at[other], stats_all.at[other], gather_send.at[o], gather_sem.at[other], freq=other
            ).wait_recv()
        rows = [stats_all[:, i].reshape(freq_count * blocks, LANES) for i in range(3)]
        solved[...] = solve(weight, *rows, matrix, square, lags).reshape(freq_count, blocks, LANES)
        taps[me] = solved[layer]
        for o in range(1, trace_count):
            taps_copy(o).start()

    def take_taps(s):
        @pl.when(me != s)
        def _():
            remote(taps.at[s], taps.at[s], taps_send.at[0], taps_sem.at[s], trace=s).wait_recv()

        own = taps[s]
        filters_out[s, 0] = own[:, :TAPS]
        filters_out[s, 1] = turn(own, TAPS)[:, :TAPS]

    at_once = 2 if shots % 2 == 0 else 1

    def finish(i, carry):
        group = [i * at_once + s for s in range(at_once)]
        for s in group:
            take_taps(s)
        shaped = shapes(taps[pl.ds(i * at_once, at_once)], table)
        for s in range(at_once):
            shaped_back(shaped[s], rec, spec, table, group[s])
        for s in group:
            local(rec, out_any, out_sem, s).start()
        return carry

    relay_at = jnp.minimum(me, 2)

    def measure_step(s, carry):
        measure(s)
        pl.when(owns & (s == relay_at))(relay)
        return carry

    table_copy.wait()
    lax.fori_loop(0, shots, measure_step, 0)

    @pl.when(owns)
    def _():
        gather()
        prepare()
        solve_own()

    lax.fori_loop(0, shots // at_once, finish, 0)

    def drain(s, carry):
        for side in range(2):

            @pl.when(sends[side] & jnp.logical_not(detoured(side, s)))
            def _():
                halo_copy(side, s).wait_send()

            @pl.when(detoured(side, s))
            def _():
                detour_copy(side, s).wait_send()

            @pl.when(passes[side] & (s < detours))
            def _():
                pass_copy(side, jnp.minimum(s, detours - 1)).wait_send()

        for end, where in ends:

            @pl.when((me == where) & (s != where))
            def _():
                corner_copy(end, s, s).wait_send()

        @pl.when(me != s)
        def _():
            stats_copy(s).wait_send()

        local(rec, out_any, out_sem, s).wait()
        return carry

    lax.fori_loop(0, shots, drain, 0)

    @pl.when(owns)
    def _():
        for o in range(1, freq_count):
            relay_copy(o).wait_send()
            gather_copy(o).wait_send()
        for o in range(1, trace_count):
            taps_copy(o).wait_send()


def body(recorded, multiples):
    shots, parts, freq_rows, trace_rows = multiples.shape
    blocks = freq_rows // FB
    trace_count, freq_count = lax.axis_size("trace"), lax.axis_size("freq")
    assert shots <= trace_count
    weight = 0.5 * FB * trace_rows * trace_count
    pack_rows = freq_rows * HALF // LANES
    detours = detour_count(shots, trace_count)
    run = TAPS * freq_count * blocks // LANES

    table, runs = all_tables()
    field = (shots, parts, freq_rows, trace_rows)
    dma = pltpu.SemaphoreType.DMA
    vmem = pl.BlockSpec(memory_space=pltpu.VMEM)
    anywhere = pl.BlockSpec(memory_space=pl.ANY)
    return pl.pallas_call(
        functools.partial(fit_kernel, weight, trace_count, freq_count, runs),
        in_specs=[anywhere, anywhere, anywhere],
        out_specs=[anywhere, vmem],
        out_shape=[
            jax.ShapeDtypeStruct(field, F32),
            jax.ShapeDtypeStruct((shots, parts, blocks, TAPS), F32),
        ],
        scratch_shapes=[
            pltpu.VMEM(field, F32),
            pltpu.VMEM(field, F32),
            pltpu.VMEM((2, shots, parts, pack_rows, LANES), F32),
            pltpu.VMEM((2, shots, parts, pack_rows, LANES), F32),
            pltpu.VMEM((shots, 4, freq_rows, LANES), F32),
            pltpu.VMEM((6, blocks, LANES), F32),
            pltpu.VMEM((shots, HALF // 2, blocks, LANES), F32),
            pltpu.VMEM((2, HALF // 2, blocks, LANES), F32),
            pltpu.VMEM((freq_count, HALF, blocks, LANES), F32),
            pltpu.VMEM((shots, 3, blocks, LANES), F32),
            pltpu.VMEM((trace_count, 3, blocks, LANES), F32),
            pltpu.VMEM((freq_count, 3, blocks, LANES), F32),
            pltpu.VMEM((shots, blocks, LANES), F32),
            pltpu.VMEM((freq_count, blocks, LANES), F32),
            pltpu.VMEM((TAPS + 2, freq_count * blocks, LANES), F32),
            pltpu.VMEM((run, LANES, LANES), F32),
            pltpu.VMEM((2, run + TAPS, LANES), F32),
            pltpu.VMEM(table.shape, BF16),
            pltpu.VMEM((freq_rows, LANES), BF16),
            pltpu.VMEM((max(detours, 1), parts, pack_rows, LANES), F32),
            dma((max(detours, 1),)),
            dma((max(detours, 1),)),
            dma,
            dma((shots,)),
            dma((shots,)),
            dma((shots,)),
            dma((2, shots)),
            dma((2, shots)),
            dma((shots,)),
            dma((2,)),
            dma((freq_count,)),
            dma((freq_count,)),
            dma((shots,)),
            dma((trace_count,)),
            dma((freq_count,)),
            dma((freq_count,)),
            dma((trace_count,)),
            dma((shots,)),
        ],
        compiler_params=pltpu.CompilerParams(
            collective_id=0, has_side_effects=True, vmem_limit_bytes=48000000
        ),
        name="fit",
    )(multiples, recorded, jnp.asarray(table))


def solution(mesh):
    spec = P(None, None, "freq", "trace")
    return jax.shard_map(
        body,
        mesh=mesh,
        in_specs=(spec, spec),
        out_specs=(spec, P(None, None, "freq", None)),
        check_vma=False,
    )
```

```python
import functools

import jax
import jax.numpy as jnp
import numpy as np
from jax import lax
from jax.experimental import pallas as pl
from jax.experimental.pallas import tpu as pltpu
from jax.sharding import PartitionSpec as P

FB = 64
TAPS = 64
ITERS = 3
HALF = TAPS // 2
LANES = 128
POINTS = 2 * LANES
F32 = jnp.float32
BF16 = jnp.bfloat16
MESH = pl.DeviceIdType.MESH


def lanes_of(shape):
    return lax.broadcasted_iota(jnp.int32, shape, len(shape) - 1)


def turn(value, shift):
    shift = shift % LANES
    return value if shift == 0 else pltpu.roll(value, shift, 1)


def split(value):
    high = value.astype(BF16)
    return high, (value - high.astype(F32)).astype(BF16)


def waves(positions):
    phase = (2 * np.pi / POINTS) * np.outer(np.asarray(positions), np.arange(LANES) + 0.5)
    return np.cos(phase), np.sin(phase)


def both_waves(positions):
    return np.concatenate(waves(positions), 1)


def halves(table):
    high = table.astype(np.float32).astype(BF16)
    return high, (table - high.astype(np.float64)).astype(np.float32).astype(BF16)


def all_tables():
    high, low = halves(both_waves(np.arange(LANES)))
    tail_high, tail_low = halves(both_waves(LANES + np.arange(TAPS)))
    lag = np.where(np.arange(LANES) < TAPS, np.arange(LANES), LANES - np.arange(LANES))
    used = (np.arange(LANES) != TAPS) / LANES
    sign = np.where(np.arange(LANES) < TAPS, -2.0, 2.0)
    lag_cos, lag_sin = waves(lag)
    right = both_waves(-1 - np.arange(TAPS)).T / LANES
    none = np.zeros_like(right)
    shape_high, shape_low = halves(both_waves(np.arange(TAPS)))
    parts = dict(
        wide=[high, high],
        low=[low],
        tail=[tail_high, tail_high, tail_low, np.zeros_like(tail_low)],
        power=[np.concatenate(halves(lag_cos.T * used), 1)],
        cross=[np.concatenate(halves(lag_sin.T * (sign * used)), 1)],
        sides=[np.concatenate(halves(np.block([[right, none], [none, right]])), 1)],
        shape=[shape_high, shape_high, shape_low, np.zeros_like(shape_low)],
        back=[np.concatenate(halves(both_waves(TAPS + np.arange(LANES)).T / LANES), 1)],
    )
    parts = {name: np.concatenate(part, 0) for name, part in parts.items()}
    runs, start = {}, 0
    for name, part in parts.items():
        runs[name] = slice(start, start + part.shape[0])
        start += part.shape[0]
    return np.concatenate(list(parts.values()), 0), runs


def over_first(left, right):
    return lax.dot_general(left, right, (((0,), (0,)), ((), ())), preferred_element_type=F32)


def product(left, right):
    return jnp.dot(left, right, preferred_element_type=F32)


def exact(left, right):
    return jnp.dot(left, right, precision=lax.Precision.HIGHEST, preferred_element_type=F32)


def mirror(total):
    rows = lax.broadcasted_iota(jnp.int32, (LANES, LANES), 0)
    return (rows + lanes_of((LANES, LANES)) == total).astype(F32)


def total_of(value):
    return jnp.sum(jnp.sum(value, axis=0, keepdims=True), axis=1, keepdims=True)


def column_sum(value):
    return jnp.sum(value, axis=0, keepdims=True)


def pack_edges(m, edge, s):
    freq_rows = m.shape[2]
    groups = LANES // HALF
    rows = freq_rows // groups
    lane = lanes_of((rows, LANES))
    for part in range(2):
        for side in range(2):
            packed = None
            for g in range(groups):
                shift = HALF * g + HALF if side == 0 else HALF * g
                value = turn(m[s, part, g * rows : (g + 1) * rows, :], shift)
                packed = value if packed is None else jnp.where(lane >= HALF * g, value, packed)
            edge[side, s, part] = packed


def corners(m, ends, corner, s, at_last):
    freq_rows = m.shape[2]
    wide = (freq_rows, LANES)
    lane = lanes_of(wide)
    real = pltpu.roll(m[s, 0], jnp.where(at_last, HALF, 0), 1)
    imag = pltpu.roll(m[s, 1], jnp.where(at_last, 2 * HALF, HALF), 1)
    both = jnp.where(lane < HALF, real, imag)
    rest = both - both.astype(BF16).astype(F32)
    ends[...] = jnp.where(lane < TAPS, both, turn(rest, TAPS)).astype(BF16)
    lane = lanes_of((HALF, LANES))
    for b in range(freq_rows // FB):
        part = ends[b * FB : (b + 1) * FB, :]
        gram = over_first(part, part)
        gram = gram[:TAPS] + gram[TAPS:]
        gram = gram + turn(gram, TAPS)
        one, two = gram[:HALF], turn(gram[HALF:], HALF)
        value = jnp.where(lane % TAPS < HALF, one + two, one - two)
        corner[s, :, b, :] = jnp.where(
            lane[: HALF // 2] < TAPS, value[: HALF // 2], value[HALF // 2 :]
        )


def joined_corners(left, right):
    shape = left.shape
    lane = lanes_of(shape)

    def moved(value, shift):
        return pltpu.roll(value, shift % LANES, 2)

    def pick(*values):
        result = values[0]
        for i in range(1, 4):
            result = jnp.where(lane >= i * HALF, values[i], result)
        return result

    first = pick(right, moved(left, HALF), moved(right, HALF), moved(left, TAPS))
    second = pick(moved(right, TAPS), moved(left, -HALF), moved(right, -HALF), left)
    value = jnp.concatenate([first, second], 0)
    place = lanes_of(value.shape) % TAPS
    step = 1
    while step < HALF:
        none = jnp.zeros((step,) + shape[1:], F32)
        later = jnp.concatenate([moved(value[step:], -step), none], 0)
        sooner = jnp.concatenate([none, moved(value[:-step], step)], 0)
        value = value + jnp.where(
            place < HALF - step, later, jnp.where(place >= HALF + step, sooner, 0.0)
        )
        step *= 2
    return value


def fourfold(value, table):
    count = value.shape[0]
    both = product(jnp.concatenate(split(value), 0), table)
    both = both[:count] + both[count:]
    return both[:, :LANES] + both[:, LANES:]


def threefold(value, table):
    top = value.astype(BF16)
    rest = turn(value - top.astype(F32), TAPS)
    mixed = jnp.where(lanes_of(value.shape) < TAPS, value, rest).astype(BF16)
    return product(jnp.concatenate([mixed, top], 1), table)


def statistics(m, rec, halo, spec, sums, table, s):
    freq_rows = m.shape[2]
    group_rows = freq_rows * HALF // LANES
    lane = lanes_of((FB, LANES))
    for b in range(freq_rows // FB):
        rows = slice(b * FB, (b + 1) * FB)
        group, first = (b * FB) // group_rows, (b * FB) % group_rows
        near = slice(first, first + FB)
        starts, tails = [], []
        for part in range(2):
            turned = turn(m[s, part, rows, :], HALF)
            left = turn(halo[0, s, part, near, :], -HALF * group)
            right = turn(halo[1, s, part, near, :], HALF - HALF * group)
            starts.append(jnp.where(lane < HALF, left, turned))
            tails.append(jnp.where(lane < HALF, turned, right))
        high, rest = split(jnp.concatenate(starts + [rec[s, 0, rows, :], rec[s, 1, rows, :]], 0))
        main = product(jnp.concatenate([high, rest], 1), table("wide")) + product(high, table("low"))
        last = threefold(jnp.concatenate(tails, 0), table("tail"))

        def parts(value, first):
            return value[first : first + FB, :LANES], value[first : first + FB, LANES:]

        s_all = parts(main, 0) + parts(main, FB)
        t_all = parts(last, 0) + parts(last, FB)
        r_ac, r_as, r_bc, r_bs = parts(main, 2 * FB) + parts(main, 3 * FB)
        w_all = [x + y for x, y in zip(s_all, t_all)]
        for i in range(4):
            spec[s, i, rows, :] = w_all[i]
        w_ac, w_as, w_bc, w_bs = w_all
        t_ac, t_as, t_bc, t_bs = t_all
        power = sum(x * (w + t) for x, w, t in zip(s_all, w_all, t_all))
        cross = (w_ac * w_bs - w_as * w_bc) - (t_ac * t_bs - t_as * t_bc)
        found = [
            power,
            cross,
            w_ac * r_ac + w_as * r_as + w_bc * r_bc + w_bs * r_bs,
            w_ac * r_as - w_as * r_ac + w_bc * r_bs - w_bs * r_bc,
            w_ac * r_bc + w_as * r_bs - w_bc * r_ac - w_bs * r_as,
            w_ac * r_bs - w_as * r_bc - w_bc * r_as + w_bs * r_ac,
        ]
        for i in range(6):
            sums[i, b : b + 1, :] = column_sum(found[i])


def prepare_corners(corner, matrix):
    blocks = corner.shape[0] * corner.shape[2]

    def row(r):
        return corner[:, r, :, :].reshape(blocks, LANES)

    lane = lanes_of((blocks, LANES))
    place = lane % TAPS
    is_real = lane < TAPS
    for i in range(HALF):
        value = row(i)
        if i:
            moved = jnp.where(place < HALF - 1, turn(value, -1), 0.0)
            matrix[i - 1] = jnp.where(is_real, -moved, moved)
        value = jnp.where(place < HALF, 0.0, value)
        matrix[HALF + i] = jnp.where(is_real, -value, value)
    matrix[HALF - 1] = jnp.zeros((blocks, LANES), F32)
    right = jnp.where(place < HALF, row(0), 0.0)
    add_real = jnp.where(lane < HALF, right, 0.0)
    add_imag = jnp.where(lane < HALF, turn(right, TAPS), 0.0)
    back = mirror(LANES)
    matrix[TAPS] = jnp.where(is_real, add_real, exact(add_real, back))
    matrix[TAPS + 1] = jnp.where(is_real, -add_imag, exact(add_imag, back))


def turn_matrix(matrix, square):
    groups = LANES // matrix.shape[1]
    run = TAPS // groups
    for k in range(run):
        square[k] = jnp.concatenate([matrix[g * run + k] for g in range(groups)], 0).T


def solve(weight, toep_real, toep_imag, gradient, matrix, square, lags):
    blocks = gradient.shape[0]
    groups = LANES // blocks
    run = TAPS // groups
    toep_real = toep_real + matrix[TAPS]
    toep_imag = toep_imag + matrix[TAPS + 1]
    for i, toep in enumerate((toep_real, toep_imag)):
        base = jnp.concatenate([turn(toep, g * run) for g in range(groups)], 0).T
        lags[i, :run] = base[LANES - run :]
        lags[i, run:] = base[:TAPS]
    for k in range(run):
        square[k, :TAPS] += lags[0, run - k : run - k + TAPS]
        square[k, TAPS:] += lags[1, run - k : run - k + TAPS]

    shape = (LANES, LANES)
    place = lanes_of(shape) % blocks
    lane = lanes_of((run, LANES))

    def grouped(rows):
        result = rows[:run]
        for g in range(1, groups):
            result = jnp.where(lane >= g * blocks, rows[g * run : (g + 1) * run], result)
        return result

    gradient = jnp.concatenate([gradient] * groups, 0).T
    filters = jnp.zeros(shape, F32)
    direction = norm_now = None
    for iteration in range(ITERS):
        norm_next = total_of(gradient * gradient) * (1.0 / groups)
        if iteration == 0:
            direction = gradient
        else:
            direction = gradient + (norm_next / norm_now) * direction
        norm_now = norm_next
        real, imag = grouped(direction[:TAPS]), grouped(direction[TAPS:])
        by_real = jnp.zeros(shape, F32)
        by_imag = jnp.zeros(shape, F32)
        for k in range(run):
            by_real = by_real + square[k] * real[k : k + 1]
            by_imag = by_imag + square[k] * imag[k : k + 1]
        normal = jnp.concatenate([by_real[:TAPS] - by_imag[TAPS:], by_real[TAPS:] + by_imag[:TAPS]], 0)
        shift = LANES // 2
        while shift >= blocks:
            normal = normal + turn(normal, shift)
            shift //= 2
        before = jnp.where(place == 0, 0.0, turn(direction, 1))
        after = jnp.where(place == blocks - 1, 0.0, turn(direction, -1))
        normal = normal + weight * (2.0 * direction - before - after)
        step_len = norm_now / (total_of(direction * normal) * (1.0 / groups))
        filters = filters + step_len * direction
        gradient = gradient - step_len * normal
    filters = filters.T[:blocks]
    rows = lax.broadcasted_iota(jnp.int32, (LANES, LANES), 0)
    columns = lanes_of((LANES, LANES))
    flip = (rows + columns == jnp.where(columns < TAPS, TAPS - 1, 3 * TAPS - 1)).astype(F32)
    return exact(filters, flip)


def shapes(taps, table):
    shots, blocks, _ = taps.shape
    rows = taps.reshape(shots * blocks, LANES)
    value = threefold(jnp.concatenate([rows, turn(rows, TAPS)], 0), table("shape"))
    value = jnp.concatenate([value[: shots * blocks], value[shots * blocks :]], 1)
    return value.reshape(shots, blocks, 2 * POINTS)


def shaped_back(shape, rec, spec, table, s):
    for b in range(rec.shape[2] // FB):
        rows = slice(b * FB, (b + 1) * FB)
        w_ac, w_as, w_bc, w_bs = [spec[s, i, rows, :] for i in range(4)]
        h_ac, h_as, h_bc, h_bs = [shape[b : b + 1, i * LANES : (i + 1) * LANES] for i in range(4)]
        y_ac = h_ac * w_ac - h_as * w_as - h_bc * w_bc + h_bs * w_bs
        y_as = h_ac * w_as + h_as * w_ac - h_bc * w_bs - h_bs * w_bc
        y_bc = h_ac * w_bc - h_as * w_bs + h_bc * w_ac - h_bs * w_as
        y_bs = h_ac * w_bs + h_as * w_bc + h_bc * w_as + h_bs * w_ac
        both = jnp.concatenate(
            [jnp.concatenate([y_ac, y_as], 1), jnp.concatenate([y_bc, y_bs], 1)], 0
        )
        applied = fourfold(both, table("back"))
        rec[s, 0, rows, :] = rec[s, 0, rows, :] - applied[:FB]
        rec[s, 1, rows, :] = rec[s, 1, rows, :] - applied[FB:]


def detour_count(shots, trace_count):
    return max((shots - 2) // 2, 0) if trace_count >= 4 else 0


def fit_kernel(
    weight,
    trace_count,
    freq_count,
    runs,
    m_any,
    rec_any,
    table_any,
    out_any,
    filters_out,
    m,
    rec,
    edge,
    halo,
    spec,
    sums,
    corner,
    corner_in,
    corner_all,
    stats,
    stats_in,
    stats_all,
    taps,
    solved,
    matrix,
    square,
    lags,
    tables,
    ends_v,
    passing,
    pass_send,
    pass_sem,
    table_sem,
    m_sem,
    rec_sem,
    out_sem,
    edge_send,
    halo_sem,
    corner_send,
    corner_sem,
    relay_send,
    relay_sem,
    stats_send,
    stats_sem,
    gather_send,
    gather_sem,
    taps_send,
    taps_sem,
):
    shots = m.shape[0]
    blocks = m.shape[2] // FB
    last = trace_count - 1
    me = lax.axis_index("trace")
    layer = lax.axis_index("freq")
    owns = me < shots
    ends = ((0, 0), (1, last))

    def remote(source, target, send, arrive, **where):
        return pltpu.make_async_remote_copy(
            src_ref=source,
            dst_ref=target,
            send_sem=send,
            recv_sem=arrive,
            device_id=where,
            device_id_type=MESH,
        )

    def local(source, target, sem, s):
        return pltpu.make_async_copy(source.at[s], target.at[s], sem.at[s])

    for s in range(shots):
        local(m_any, m, m_sem, s).start()
    table_copy = pltpu.make_async_copy(table_any, tables, table_sem)
    table_copy.start()
    for s in range(shots):
        local(rec_any, rec, rec_sem, s).start()

    def table(name):
        return tables[runs[name], :]

    barrier = pltpu.get_barrier_semaphore()
    for o in range(1, trace_count):
        pl.semaphore_signal(
            barrier, inc=1, device_id={"trace": lax.rem(me + o, trace_count)}, device_id_type=MESH
        )
    for o in range(1, freq_count):
        pl.semaphore_signal(
            barrier, inc=1, device_id={"freq": lax.rem(layer + o, freq_count)}, device_id_type=MESH
        )

    @pl.when(me == 0)
    def _():
        halo[0] = jnp.zeros(halo.shape[1:], F32)

    @pl.when(me == last)
    def _():
        halo[1] = jnp.zeros(halo.shape[1:], F32)

    pl.semaphore_wait(barrier, trace_count + freq_count - 2)

    def halo_copy(side, s):
        other = jnp.minimum(me + 1, last) if side == 0 else jnp.maximum(me - 1, 0)
        return remote(
            edge.at[side, s], halo.at[side, s], edge_send.at[side, s], halo_sem.at[side, s], trace=other
        )

    def corner_copy(end, s, owner):
        return remote(corner.at[s], corner_in.at[end], corner_send.at[s], corner_sem.at[end], trace=owner)

    def relay_copy(o):
        return remote(
            corner_all.at[layer],
            corner_all.at[layer],
            relay_send.at[o],
            relay_sem.at[layer],
            freq=lax.rem(layer + o, freq_count),
        )

    def stats_copy(s):
        return remote(stats.at[s], stats_in.at[me], stats_send.at[s], stats_sem.at[me], trace=s)

    def gather_copy(o):
        return remote(
            stats_all.at[layer],
            stats_all.at[layer],
            gather_send.at[o],
            gather_sem.at[layer],
            freq=lax.rem(layer + o, freq_count),
        )

    def taps_copy(o):
        return remote(
            taps.at[me], taps.at[me], taps_send.at[o], taps_sem.at[me], trace=lax.rem(me + o, trace_count)
        )

    sends = (me < last, me > 0)
    receives = (me > 0, me < last)

    middle = trace_count // 2
    detours = detour_count(shots, trace_count)

    def detoured(side, s):
        if not detours:
            return False
        return (me == (middle - 1 if side == 0 else middle)) & (s > 1) & (lax.rem(s, 2) == 1)

    def detour_copy(side, s):
        i = jnp.maximum(s - 3, 0) // 2
        return remote(
            edge.at[side, s],
            passing.at[i],
            edge_send.at[side, s],
            pass_sem.at[i],
            trace=last if side == 0 else 0,
        )

    def pass_copy(side, i):
        s = 2 * i + 3
        return remote(
            passing.at[i],
            halo.at[side, s],
            pass_send.at[i],
            halo_sem.at[side, s],
            trace=middle if side == 0 else middle - 1,
        )

    passes = (me == last, me == 0)

    def start_halo(s):
        for side in range(2):

            @pl.when(sends[side] & jnp.logical_not(detoured(side, s)))
            def _():
                halo_copy(side, s).start()

            @pl.when(detoured(side, s))
            def _():
                detour_copy(side, s).start()

    def pass_on(i):
        for side in range(2):

            @pl.when(passes[side])
            def _():
                detour_copy(side, 2 * i + 3).wait_recv()
                pass_copy(side, i).start()

    def send_edges(s, carry):
        local(m_any, m, m_sem, s).wait()
        pack_edges(m, edge, s)
        start_halo(s)
        return carry

    lax.fori_loop(0, shots, send_edges, 0)
    @pl.when((me == 0) | (me == last))
    def _():
        def send_corners(s, carry):
            corners(m, ends_v, corner, s, me == last)
            for end, where in ends:

                @pl.when((me == where) & (s != where))
                def _():
                    corner_copy(end, s, s).start()

                @pl.when((me == where) & (s == where))
                def _():
                    corner_in[end] = corner[s]

            return carry

        lax.fori_loop(0, shots, send_corners, 0)

    for i in range(detours):
        pass_on(i)

    def measure(s):
        local(rec_any, rec, rec_sem, s).wait()
        for side in range(2):

            @pl.when(receives[side])
            def _():
                halo_copy(side, s).wait_recv()

        statistics(m, rec, halo, spec, sums, table, s)
        stats[s, 0] = fourfold(sums[0], table("power"))
        stats[s, 1] = fourfold(sums[1], table("cross"))
        stats[s, 2] = fourfold(jnp.concatenate([sums[i] for i in range(2, 6)], 1), table("sides"))

        @pl.when(me != s)
        def _():
            stats_copy(s).start()

    def relay():
        for end, where in ends:

            @pl.when(me != where)
            def _():
                corner_copy(end, 0, me).wait_recv()

        corner_all[layer] = joined_corners(corner_in[0], corner_in[1])
        for o in range(1, freq_count):
            relay_copy(o).start()

    def prepare():
        for o in range(1, freq_count):
            other = lax.rem(layer + o, freq_count)
            remote(
                corner_all.at[other], corner_all.at[other], relay_send.at[o], relay_sem.at[other], freq=other
            ).wait_recv()
        prepare_corners(corner_all, matrix)
        turn_matrix(matrix, square)

    def gather():
        whole = stats[me]
        for o in range(1, trace_count):
            other = lax.rem(me + o, trace_count)
            remote(
                stats.at[0], stats_in.at[other], stats_send.at[0], stats_sem.at[other], trace=other
            ).wait_recv()
            whole = whole + stats_in[other]
        stats_all[layer] = whole
        for o in range(1, freq_count):
            gather_copy(o).start()

    def solve_own():
        for o in range(1, freq_count):
            other = lax.rem(layer + o, freq_count)
            remote(
                stats_all.at[other], stats_all.at[other], gather_send.at[o], gather_sem.at[other], freq=other
            ).wait_recv()
        rows = [stats_all[:, i].reshape(freq_count * blocks, LANES) for i in range(3)]
        solved[...] = solve(weight, *rows, matrix, square, lags).reshape(freq_count, blocks, LANES)
        taps[me] = solved[layer]
        for o in range(1, trace_count):
            taps_copy(o).start()

    def take_taps(s):
        @pl.when(me != s)
        def _():
            remote(taps.at[s], taps.at[s], taps_send.at[0], taps_sem.at[s], trace=s).wait_recv()

        own = taps[s]
        filters_out[s, 0] = own[:, :TAPS]
        filters_out[s, 1] = turn(own, TAPS)[:, :TAPS]

    at_once = 2 if shots % 2 == 0 else 1

    def finish(i, carry):
        group = [i * at_once + s for s in range(at_once)]
        for s in group:
            take_taps(s)
        shaped = shapes(taps[pl.ds(i * at_once, at_once)], table)
        for s in range(at_once):
            shaped_back(shaped[s], rec, spec, table, group[s])
        for s in group:
            local(rec, out_any, out_sem, s).start()
        return carry

    relay_at = jnp.minimum(me, 2)

    def measure_step(s, carry):
        measure(s)
        pl.when(owns & (s == relay_at))(relay)
        return carry

    table_copy.wait()
    lax.fori_loop(0, shots, measure_step, 0)

    @pl.when(owns)
    def _():
        gather()
        prepare()
        solve_own()

    lax.fori_loop(0, shots // at_once, finish, 0)

    def drain(s, carry):
        for side in range(2):

            @pl.when(sends[side] & jnp.logical_not(detoured(side, s)))
            def _():
                halo_copy(side, s).wait_send()

            @pl.when(detoured(side, s))
            def _():
                detour_copy(side, s).wait_send()

            @pl.when(passes[side] & (s < detours))
            def _():
                pass_copy(side, jnp.minimum(s, detours - 1)).wait_send()

        for end, where in ends:

            @pl.when((me == where) & (s != where))
            def _():
                corner_copy(end, s, s).wait_send()

        @pl.when(me != s)
        def _():
            stats_copy(s).wait_send()

        local(rec, out_any, out_sem, s).wait()
        return carry

    lax.fori_loop(0, shots, drain, 0)

    @pl.when(owns)
    def _():
        for o in range(1, freq_count):
            relay_copy(o).wait_send()
            gather_copy(o).wait_send()
        for o in range(1, trace_count):
            taps_copy(o).wait_send()


def body(recorded, multiples):
    shots, parts, freq_rows, trace_rows = multiples.shape
    blocks = freq_rows // FB
    trace_count, freq_count = lax.axis_size("trace"), lax.axis_size("freq")
    assert shots <= trace_count
    weight = 0.5 * FB * trace_rows * trace_count
    pack_rows = freq_rows * HALF // LANES
    detours = detour_count(shots, trace_count)
    run = TAPS * freq_count * blocks // LANES

    table, runs = all_tables()
    field = (shots, parts, freq_rows, trace_rows)
    dma = pltpu.SemaphoreType.DMA
    vmem = pl.BlockSpec(memory_space=pltpu.VMEM)
    anywhere = pl.BlockSpec(memory_space=pl.ANY)
    return pl.pallas_call(
        functools.partial(fit_kernel, weight, trace_count, freq_count, runs),
        in_specs=[anywhere, anywhere, anywhere],
        out_specs=[anywhere, vmem],
        out_shape=[
            jax.ShapeDtypeStruct(field, F32),
            jax.ShapeDtypeStruct((shots, parts, blocks, TAPS), F32),
        ],
        scratch_shapes=[
            pltpu.VMEM(field, F32),
            pltpu.VMEM(field, F32),
            pltpu.VMEM((2, shots, parts, pack_rows, LANES), F32),
            pltpu.VMEM((2, shots, parts, pack_rows, LANES), F32),
            pltpu.VMEM((shots, 4, freq_rows, LANES), F32),
            pltpu.VMEM((6, blocks, LANES), F32),
            pltpu.VMEM((shots, HALF // 2, blocks, LANES), F32),
            pltpu.VMEM((2, HALF // 2, blocks, LANES), F32),
            pltpu.VMEM((freq_count, HALF, blocks, LANES), F32),
            pltpu.VMEM((shots, 3, blocks, LANES), F32),
            pltpu.VMEM((trace_count, 3, blocks, LANES), F32),
            pltpu.VMEM((freq_count, 3, blocks, LANES), F32),
            pltpu.VMEM((shots, blocks, LANES), F32),
            pltpu.VMEM((freq_count, blocks, LANES), F32),
            pltpu.VMEM((TAPS + 2, freq_count * blocks, LANES), F32),
            pltpu.VMEM((run, LANES, LANES), F32),
            pltpu.VMEM((2, run + TAPS, LANES), F32),
            pltpu.VMEM(table.shape, BF16),
            pltpu.VMEM((freq_rows, LANES), BF16),
            pltpu.VMEM((max(detours, 1), parts, pack_rows, LANES), F32),
            dma((max(detours, 1),)),
            dma((max(detours, 1),)),
            dma,
            dma((shots,)),
            dma((shots,)),
            dma((shots,)),
            dma((2, shots)),
            dma((2, shots)),
            dma((shots,)),
            dma((2,)),
            dma((freq_count,)),
            dma((freq_count,)),
            dma((shots,)),
            dma((trace_count,)),
            dma((freq_count,)),
            dma((freq_count,)),
            dma((trace_count,)),
            dma((shots,)),
        ],
        compiler_params=pltpu.CompilerParams(
            collective_id=0, has_side_effects=True, vmem_limit_bytes=48000000
        ),
        name="fit",
    )(multiples, recorded, jnp.asarray(table))


def solution(mesh):
    spec = P(None, None, "freq", "trace")
    return jax.shard_map(
        body,
        mesh=mesh,
        in_specs=(spec, spec),
        out_specs=(spec, P(None, None, "freq", None)),
        check_vma=False,
    )
```
